256 devices in a mesh: tm: 128 (over z_hi, y, x, core), rows: 2 (over z_lo).
Axes of the slice: x: 4, y: 4, z: 8 (z_hi: 4, z_lo: 2; z = z_hi * 2 + z_lo), core: 2. Of those that a mesh axis runs over, the one named last changes fastest.
Arguments:
- resid: float32 [2, 128, 16, 512], P(None, 'tm', 'rows'), may hold values from -3 to 3
- basis: float32 [4, 2, 128, 16, 512], P(None, None, 'tm', 'rows'), may hold values from -0.0041432036 to 0.0041432036
Outputs:
- precond: float32 [2, 128, 16, 512], P(None, 'tm', 'rows')
- image: float32 [2, 128, 16, 512], P(None, 'tm', 'rows')
- gram: float32 [5], replicated
The draws below stay inside these ranges and needn't reach their ends.
All inputs are finite; a program needn't handle non-finite values.
Results may differ from the reference program's by a relative error of at most 0.0005.
Values sent between devices are 32-bit elements; how exact they have to be, the bound alone decides.
No kernel may reach another device: no remote copies, remote signals or barrier semaphores. Data moves between devices by JAX's collectives and lax.ppermute only.
A program may use at most 64 MiB of HBM per device.

```python
import jax
import jax.numpy as jnp

NY = 512
SWEEPS = 4
KRYLOV = 4
STEPS = 128
NX = 16


def block_scale(key, extent, pieces, low, top_value):
    loudness, own = 1.0, jax.random.fold_in(key, 6)
    for axis_at, shards_of in pieces:
        heights = jnp.exp(jax.random.uniform(jax.random.fold_in(own, axis_at), (shards_of,), jnp.float32, low / len(pieces), top_value / len(pieces)))
        loudness = loudness * jnp.repeat(heights, extent[axis_at] // shards_of).reshape([-1 if axis == axis_at else 1 for axis in range(len(extent))])
    return loudness


def centred(own_key, shape, spread, bound, shards=(), held_as=jnp.bfloat16):
    array = spread * jax.random.normal(own_key, shape, jnp.float32)
    if shards:
        array = array * block_scale(own_key, shape, shards, -0.22, 0.18)
    return jnp.clip(array, -bound, bound).astype(held_as)


def setup_inputs(seed: int = 0) -> dict:
    key_of = jax.random.split(jax.random.key(seed), 3)
    resid = centred(key_of[0], (2, STEPS, NX, NY), 0.5, 3.0, ((1, 128), (2, 2)), jnp.float32)
    basis = centred(key_of[1], (KRYLOV, 2, STEPS, NX, NY), (1.0 / (2 * STEPS * NX * NY) ** 0.5), 0.0041432036, ((2, 128), (3, 2)), jnp.float32)
    return {"resid": resid, "basis": basis}


ALPHA = 0.01


def neighbours(field):
    padded = jnp.pad(field, ((0, 0), (1, 1), (1, 1)))
    return padded[:, 2:, 1:-1] + padded[:, :-2, 1:-1] + padded[:, 1:-1, 2:] + padded[:, 1:-1, :-2]


def reference(resid, basis):
    steps = resid.shape[1]
    coupling = 16.0 / (steps * steps)
    index = jnp.arange(steps).astype(jnp.float32)
    gamma = jnp.power(jnp.float32(ALPHA), index / steps)
    scaled = resid * gamma[None, :, None, None]
    rhat = jnp.fft.fft(scaled, axis=1)
    base = jnp.power(jnp.float32(ALPHA), jnp.float32(1.0) / steps)
    lam = 1.0 - base * jnp.exp(-2j * jnp.pi * index / steps)
    lam = lam[:, None, None]
    right = lam * rhat[0] + rhat[1]
    denom = lam * lam + 4.0 * coupling
    uhat = right / denom
    for sweep in range(SWEEPS - 1):
        uhat = (right + coupling * neighbours(uhat)) / denom
    vhat = lam * uhat - rhat[0]
    yhat = jnp.stack([uhat, vhat])
    precond = jnp.real(jnp.fft.ifft(yhat, axis=1)) / gamma[None, :, None, None]
    earlier = jnp.pad(precond, ((0, 0), (1, 0), (0, 0), (0, 0)))[:, :-1]
    first = precond[0] - earlier[0] - precond[1]
    second = precond[1] - earlier[1] - coupling * (neighbours(precond[0]) - 4.0 * precond[0])
    image = jnp.stack([first, second])
    inner = jnp.sum(basis * image[None], axis=(1, 2, 3, 4))
    total = jnp.sum(image * image) / image.size
    gram = jnp.concatenate([inner, total[None]])
    return precond, image, gram
```

```python
import jax
import jax.numpy as jnp
import numpy as np
from jax import lax
from jax.experimental import pallas as pl
from jax.experimental.pallas import tpu as pltpu
from jax.sharding import PartitionSpec as P

ALPHA = 0.01
SWEEPS = 4
KRYLOV = 4
LANES = 128
ROWS = 8
SLOTS = 3
BASE = 80
FIELD = 2 * ROWS
OUT = 64


def roll(value, amount, axis):
    size = value.shape[axis]
    return pltpu.roll(value, amount % size, axis)


def time_tables(steps):
    kappa = 16.0 / (steps * steps)
    index = np.arange(steps)
    gamma = ALPHA ** (index / steps)
    lam = 1.0 - ALPHA ** (1.0 / steps) * np.exp(-2j * np.pi * index / steps)
    den = lam * lam + 4.0 * kappa
    turn = np.exp(-2j * np.pi * np.outer(index, index) / steps)
    tables = []
    for m in range(SWEEPS):
        inner = np.conj(turn) @ ((1.0 / den ** (m + 1))[:, None] * turn) / steps
        tables.append(kappa**m * (inner.real / gamma[:, None]) * gamma[None, :])
    return np.concatenate(tables, 1).astype(np.float32)


def space_table(steps):
    kappa = 16.0 / (steps * steps)
    rows = 2 * ROWS
    shift = np.eye(rows, k=1) + np.eye(rows, k=-1)
    table = np.zeros((2, LANES, 2 * LANES))
    for m in range(SWEEPS + 1):
        for k in range(m + 1):
            ways = float(np.prod(np.arange(m - k + 1, m + 1)) / np.prod(np.arange(1, k + 1)))
            part = ways * np.linalg.matrix_power(shift, m - k)
            for row in range(rows):
                for out in range(rows):
                    lane = m * 4 * ROWS + (out // ROWS) * 2 * ROWS + out % ROWS
                    for c in range(2):
                        source = k * 2 * ROWS + c * ROWS + row % ROWS
                        table[row // ROWS, source, lane] = part[row, out]
    return table.reshape(2 * LANES, 2 * LANES).astype(np.float32), kappa


def lane_of(shape):
    return lax.broadcasted_iota(jnp.int32, shape, len(shape) - 1)


def packed(resid, basis):
    cols = resid.shape[-1]
    half = cols // 2
    flat = resid.reshape(2 * ROWS, cols)
    lane = lane_of(flat.shape)
    powers = [flat]
    for _ in range(SWEEPS):
        last = powers[-1]
        right = jnp.where(lane == 0, 0.0, roll(last, 1, 1))
        left = jnp.where(lane == cols - 1, 0.0, roll(last, -1, 1))
        powers.append(right + left)
    disp, velo = flat[:ROWS], flat[ROWS:]
    pair = lambda v: [v[:, :half], v[:, half:]]
    first = [p[:, :half] for p in powers] + pair(-disp) + pair(disp) + pair(velo)
    second = [p[:, half:] for p in powers]
    second.append(jnp.zeros((LANES - BASE, half), jnp.float32))
    third = []
    for c in range(2):
        for i in range(KRYLOV):
            third += pair(basis[i, c])
    return [jnp.concatenate(rows, 0).T for rows in (first, second, third)]


def delayed(value):
    row = lax.broadcasted_iota(jnp.int32, value.shape, 0)
    moved = roll(value, 1, 0)
    return jnp.where(row == 0, ALPHA * moved, moved)


def dot(left, right):
    return jnp.dot(
        left, right, precision=lax.Precision.HIGHEST, preferred_element_type=jnp.float32
    )


def solved(parts, time_table, space, kappa, count):
    steps = parts[0][0].shape[0]
    shape = (steps, LANES)
    lane = lane_of(shape)
    row = lax.broadcasted_iota(jnp.int32, shape, 0)
    is_disp = (lane & ROWS) == 0
    mixed = []
    for dc in range(2):
        sides = []
        for h in range(2):
            x = parts[h][dc]
            sides.append(jnp.where(is_disp, x - delayed(x), x))
        mixed.append(jnp.concatenate(sides, 1))
    spread = dot(jnp.concatenate(mixed, 0), space)
    both = spread[:steps] + roll(spread[steps:], ROWS, 1)
    low, high = both[:, :LANES], both[:, LANES:]
    group = 4 * ROWS
    stack = [jnp.where(lane // group == m, low, 0.0) for m in range(SWEEPS)]
    disp = dot(time_table, jnp.concatenate(stack, 0))
    disp = disp + roll(disp, 2 * group, 1)
    disp = disp + roll(disp, group, 1)
    rest = dot(time_table[:, (SWEEPS - 1) * steps :], high) * kappa
    rest = rest + roll(rest, 2 * group, 1)
    rest = rest + roll(rest, group, 1)
    late = delayed(disp)
    rate = disp - late
    edge = jnp.where(row == 0, late, 0.0)
    place = (lane - OUT) // FIELD
    outs, sums, square = [], 0.0, 0.0
    for h in range(2):
        flip = lambda v, slot: roll(v, FIELD, 1) if (slot + h) % 2 else v
        add = jnp.where(place == 0, flip(disp, 0), 0.0)
        add = jnp.where(place == 1, flip(rate, 1), add)
        add = jnp.where(place == 2, flip(edge, 2), add)
        add = jnp.where(place == 3, flip(-rest, 3), add)
        out = jnp.where(lane >= BASE, parts[h][0], 0.0) + add
        wrap = jnp.where((row == 0) & (place == 3), delayed(roll(out, 2 * FIELD, 1)), 0.0)
        out = out + wrap
        outs.append(out)
        image = jnp.where(place >= 2, out, 0.0)
        square = square + jnp.sum(image * image, 0, keepdims=True)
        turns = []
        for slot in (2, 3):
            turn = jnp.where(place == slot, out, 0.0)
            for fold in (FIELD, 2 * FIELD, 4 * FIELD):
                turn = turn + roll(turn, fold, 1)
            turns.append(turn)
        wanted = jnp.where(lane < OUT, turns[0], turns[1])
        sums = sums + jnp.sum(parts[h][2] * wanted, 0, keepdims=True)
    sums = sums + roll(sums, OUT, 1)
    sums = sums + roll(sums, -ROWS, 1)
    square = square + roll(square, FIELD, 1)
    square = square + roll(square, ROWS, 1)
    at = lane_of((1, LANES))
    square = roll(square, ROWS - (OUT + 3 * FIELD + ROWS), 1) * (1.0 / count)
    gram = jnp.where((at >= ROWS) & (at < 2 * ROWS), square, sums)
    return [jnp.where(lane < OUT, jnp.broadcast_to(gram, shape), out) for out in outs]


def gram_of(totals):
    at = lane_of(totals.shape)
    picks = [(at // FIELD == i) & (at % FIELD < ROWS) for i in range(KRYLOV)]
    picks.append((at >= ROWS) & (at < FIELD))
    return [jnp.sum(jnp.where(pick, totals, 0.0)) for pick in picks]


def pack_kernel(resid_ref, basis_ref, send_ref):
    slabs = packed(resid_ref[:, 0], basis_ref[:, :, 0])
    for slot, slab in enumerate(slabs):
        send_ref[pl.ds(slot, slab.shape[0], stride=SLOTS), :] = slab


def solve_kernel(kappa, count, recv_ref, time_ref, space_ref, send_ref):
    steps = time_ref.shape[0]
    parts = [
        [recv_ref[pl.ds(h * SLOTS + s, steps, stride=2 * SLOTS), :] for s in range(SLOTS)]
        for h in range(2)
    ]
    outs = solved(parts, time_ref[...], space_ref[...], kappa, count)
    for h, out in enumerate(outs):
        send_ref[pl.ds(h, steps, stride=2), :] = out


def unpack_kernel(recv_ref, precond_ref, image_ref, gram_ref):
    received = recv_ref[...]
    half = received.shape[0]
    turned = received.T
    for slot, (ref, c) in enumerate(
        ((precond_ref, 0), (precond_ref, 1), (image_ref, 0), (image_ref, 1))
    ):
        for dc in range(2):
            start = OUT + slot * FIELD + dc * ROWS
            ref[c, 0, :, dc * half : (dc + 1) * half] = turned[start : start + ROWS]
    for i, value in enumerate(gram_of(jnp.sum(received, 0, keepdims=True))):
        gram_ref[i] = value


def solution(mesh):
    axes = ("tm", "rows")
    steps = mesh.shape["tm"]
    devices = steps * mesh.shape["rows"]

    def on_device(resid, basis):
        cols = resid.shape[3]
        count = 2.0 * steps * 2 * ROWS * cols
        time_table = jnp.asarray(time_tables(steps))
        space, kappa = space_table(steps)
        send = pl.pallas_call(
            pack_kernel,
            out_shape=jax.ShapeDtypeStruct((devices * SLOTS, LANES), jnp.float32),
            name="pack",
        )(resid, basis)
        send = send.reshape(devices, 1, SLOTS * LANES)
        recv = lax.all_to_all(send, axes, 0, 0, tiled=True)
        recv = recv.reshape(devices * SLOTS, LANES)
        back = pl.pallas_call(
            lambda *refs: solve_kernel(kappa, count, *refs),
            out_shape=jax.ShapeDtypeStruct((devices, LANES), jnp.float32),
            name="solve",
        )(recv, time_table, jnp.asarray(space))
        home = lax.all_to_all(back, axes, 0, 0, tiled=True)
        shard = jax.ShapeDtypeStruct(resid.shape, jnp.float32)
        vmem = pl.BlockSpec(memory_space=pltpu.VMEM)
        precond, image, gram = pl.pallas_call(
            unpack_kernel,
            out_shape=(shard, shard, jax.ShapeDtypeStruct((KRYLOV + 1,), jnp.float32)),
            out_specs=(vmem, vmem, pl.BlockSpec(memory_space=pltpu.SMEM)),
            name="unpack",
        )(home)
        return precond, image, gram

    return jax.shard_map(
        on_device,
        mesh=mesh,
        in_specs=(P(None, "tm", "rows", None), P(None, None, "tm", "rows", None)),
        out_specs=(P(None, "tm", "rows", None), P(None, "tm", "rows", None), P()),
        check_vma=False,
    )
```

```python
import jax
import jax.numpy as jnp
import numpy as np
from jax import lax
from jax.experimental import pallas as pl
from jax.experimental.pallas import tpu as pltpu
from jax.sharding import PartitionSpec as P

ALPHA = 0.01
SWEEPS = 4
KRYLOV = 4
LANES = 128
ROWS = 8
SLOTS = 3
BASE = 80
FIELD = 2 * ROWS
OUT = 64


def roll(value, amount, axis):
    size = value.shape[axis]
    return pltpu.roll(value, amount % size, axis)


def time_tables(steps):
    kappa = 16.0 / (steps * steps)
    index = np.arange(steps)
    gamma = ALPHA ** (index / steps)
    lam = 1.0 - ALPHA ** (1.0 / steps) * np.exp(-2j * np.pi * index / steps)
    den = lam * lam + 4.0 * kappa
    turn = np.exp(-2j * np.pi * np.outer(index, index) / steps)
    tables = []
    for m in range(SWEEPS):
        inner = np.conj(turn) @ ((1.0 / den ** (m + 1))[:, None] * turn) / steps
        tables.append(kappa**m * (inner.real / gamma[:, None]) * gamma[None, :])
    return np.concatenate(tables, 1).astype(np.float32)


def space_table(steps):
    kappa = 16.0 / (steps * steps)
    rows = 2 * ROWS
    shift = np.eye(rows, k=1) + np.eye(rows, k=-1)
    table = np.zeros((2, LANES, 2 * LANES))
    for m in range(SWEEPS + 1):
        for k in range(m + 1):
            ways = float(np.prod(np.arange(m - k + 1, m + 1)) / np.prod(np.arange(1, k + 1)))
            part = ways * np.linalg.matrix_power(shift, m - k)
            for row in range(rows):
                for out in range(rows):
                    lane = m * 4 * ROWS + (out // ROWS) * 2 * ROWS + out % ROWS
                    for c in range(2):
                        source = k * 2 * ROWS + c * ROWS + row % ROWS
                        table[row // ROWS, source, lane] = part[row, out]
    return table.reshape(2 * LANES, 2 * LANES).astype(np.float32), kappa


def lane_of(shape):
    return lax.broadcasted_iota(jnp.int32, shape, len(shape) - 1)


def packed(resid, basis):
    cols = resid.shape[-1]
    half = cols // 2
    flat = resid.reshape(2 * ROWS, cols)
    lane = lane_of(flat.shape)
    powers = [flat]
    for _ in range(SWEEPS):
        last = powers[-1]
        right = jnp.where(lane == 0, 0.0, roll(last, 1, 1))
        left = jnp.where(lane == cols - 1, 0.0, roll(last, -1, 1))
        powers.append(right + left)
    disp, velo = flat[:ROWS], flat[ROWS:]
    pair = lambda v: [v[:, :half], v[:, half:]]
    first = [p[:, :half] for p in powers] + pair(-disp) + pair(disp) + pair(velo)
    second = [p[:, half:] for p in powers]
    second.append(jnp.zeros((LANES - BASE, half), jnp.float32))
    third = []
    for c in range(2):
        for i in range(KRYLOV):
            third += pair(basis[i, c])
    return [jnp.concatenate(rows, 0).T for rows in (first, second, third)]


def delayed(value):
    row = lax.broadcasted_iota(jnp.int32, value.shape, 0)
    moved = roll(value, 1, 0)
    return jnp.where(row == 0, ALPHA * moved, moved)


def dot(left, right):
    return jnp.dot(
        left, right, precision=lax.Precision.HIGHEST, preferred_element_type=jnp.float32
    )


def solved(parts, time_table, space, kappa, count):
    steps = parts[0][0].shape[0]
    shape = (steps, LANES)
    lane = lane_of(shape)
    row = lax.broadcasted_iota(jnp.int32, shape, 0)
    is_disp = (lane & ROWS) == 0
    mixed = []
    for dc in range(2):
        sides = []
        for h in range(2):
            x = parts[h][dc]
            sides.append(jnp.where(is_disp, x - delayed(x), x))
        mixed.append(jnp.concatenate(sides, 1))
    spread = dot(jnp.concatenate(mixed, 0), space)
    both = spread[:steps] + roll(spread[steps:], ROWS, 1)
    low, high = both[:, :LANES], both[:, LANES:]
    group = 4 * ROWS
    stack = [jnp.where(lane // group == m, low, 0.0) for m in range(SWEEPS)]
    disp = dot(time_table, jnp.concatenate(stack, 0))
    disp = disp + roll(disp, 2 * group, 1)
    disp = disp + roll(disp, group, 1)
    rest = dot(time_table[:, (SWEEPS - 1) * steps :], high) * kappa
    rest = rest + roll(rest, 2 * group, 1)
    rest = rest + roll(rest, group, 1)
    late = delayed(disp)
    rate = disp - late
    edge = jnp.where(row == 0, late, 0.0)
    place = (lane - OUT) // FIELD
    outs, sums, square = [], 0.0, 0.0
    for h in range(2):
        flip = lambda v, slot: roll(v, FIELD, 1) if (slot + h) % 2 else v
        add = jnp.where(place == 0, flip(disp, 0), 0.0)
        add = jnp.where(place == 1, flip(rate, 1), add)
        add = jnp.where(place == 2, flip(edge, 2), add)
        add = jnp.where(place == 3, flip(-rest, 3), add)
        out = jnp.where(lane >= BASE, parts[h][0], 0.0) + add
        wrap = jnp.where((row == 0) & (place == 3), delayed(roll(out, 2 * FIELD, 1)), 0.0)
        out = out + wrap
        outs.append(out)
        image = jnp.where(place >= 2, out, 0.0)
        square = square + jnp.sum(image * image, 0, keepdims=True)
        turns = []
        for slot in (2, 3):
            turn = jnp.where(place == slot, out, 0.0)
            for fold in (FIELD, 2 * FIELD, 4 * FIELD):
                turn = turn + roll(turn, fold, 1)
            turns.append(turn)
        wanted = jnp.where(lane < OUT, turns[0], turns[1])
        sums = sums + jnp.sum(parts[h][2] * wanted, 0, keepdims=True)
    sums = sums + roll(sums, OUT, 1)
    sums = sums + roll(sums, -ROWS, 1)
    square = square + roll(square, FIELD, 1)
    square = square + roll(square, ROWS, 1)
    at = lane_of((1, LANES))
    square = roll(square, ROWS - (OUT + 3 * FIELD + ROWS), 1) * (1.0 / count)
    gram = jnp.where((at >= ROWS) & (at < 2 * ROWS), square, sums)
    return [jnp.where(lane < OUT, jnp.broadcast_to(gram, shape), out) for out in outs]


def gram_of(totals):
    at = lane_of(totals.shape)
    picks = [(at // FIELD == i) & (at % FIELD < ROWS) for i in range(KRYLOV)]
    picks.append((at >= ROWS) & (at < FIELD))
    return [jnp.sum(jnp.where(pick, totals, 0.0)) for pick in picks]


def pack_kernel(resid_ref, basis_ref, send_ref):
    slabs = packed(resid_ref[:, 0], basis_ref[:, :, 0])
    for slot, slab in enumerate(slabs):
        send_ref[pl.ds(slot, slab.shape[0], stride=SLOTS), :] = slab


def solve_kernel(kappa, count, recv_ref, time_ref, space_ref, send_ref):
    steps = time_ref.shape[0]
    parts = [
        [recv_ref[pl.ds(h * SLOTS + s, steps, stride=2 * SLOTS), :] for s in range(SLOTS)]
        for h in range(2)
    ]
    outs = solved(parts, time_ref[...], space_ref[...], kappa, count)
    for h, out in enumerate(outs):
        send_ref[pl.ds(h, steps, stride=2), :] = out


def unpack_kernel(recv_ref, precond_ref, image_ref, gram_ref):
    received = recv_ref[...]
    half = received.shape[0]
    turned = received.T
    for slot, (ref, c) in enumerate(
        ((precond_ref, 0), (precond_ref, 1), (image_ref, 0), (image_ref, 1))
    ):
        for dc in range(2):
            start = OUT + slot * FIELD + dc * ROWS
            ref[c, 0, :, dc * half : (dc + 1) * half] = turned[start : start + ROWS]
    for i, value in enumerate(gram_of(jnp.sum(received, 0, keepdims=True))):
        gram_ref[i] = value


def solution(mesh):
    axes = ("tm", "rows")
    steps = mesh.shape["tm"]
    devices = steps * mesh.shape["rows"]

    params = pltpu.CompilerParams(vmem_limit_bytes=12 * 2**20)

    def on_device(resid, basis):
        cols = resid.shape[3]
        count = 2.0 * steps * 2 * ROWS * cols
        time_table = jnp.asarray(time_tables(steps))
        space, kappa = space_table(steps)
        send = pl.pallas_call(
            pack_kernel,
            out_shape=jax.ShapeDtypeStruct((devices * SLOTS, LANES), jnp.float32),
            compiler_params=params,
            name="pack",
        )(resid, basis)
        send = send.reshape(devices, 1, SLOTS * LANES)
        recv = lax.all_to_all(send, axes, 0, 0, tiled=True)
        recv = recv.reshape(devices * SLOTS, LANES)
        back = pl.pallas_call(
            lambda *refs: solve_kernel(kappa, count, *refs),
            out_shape=jax.ShapeDtypeStruct((devices, LANES), jnp.float32),
            compiler_params=params,
            name="solve",
        )(recv, time_table, jnp.asarray(space))
        home = lax.all_to_all(back, axes, 0, 0, tiled=True)
        shard = jax.ShapeDtypeStruct(resid.shape, jnp.float32)
        vmem = pl.BlockSpec(memory_space=pltpu.VMEM)
        precond, image, gram = pl.pallas_call(
            unpack_kernel,
            out_shape=(shard, shard, jax.ShapeDtypeStruct((KRYLOV + 1,), jnp.float32)),
            out_specs=(vmem, vmem, pl.BlockSpec(memory_space=pltpu.SMEM)),
            compiler_params=params,
            name="unpack",
        )(home)
        return precond, image, gram

    return jax.shard_map(
        on_device,
        mesh=mesh,
        in_specs=(P(None, "tm", "rows", None), P(None, None, "tm", "rows", None)),
        out_specs=(P(None, "tm", "rows", None), P(None, "tm", "rows", None), P()),
        check_vma=False,
    )
```

```python
import math

import jax
import jax.numpy as jnp
import numpy as np
from jax import lax
from jax.experimental import pallas as pl
from jax.experimental.pallas import tpu as pltpu
from jax.sharding import PartitionSpec as P

ALPHA = 0.01
SWEEPS = 4
KRYLOV = 4
LANES = 128
ROWS = 8
SLOTS = 2
FIELD = 2 * ROWS
OUT = 64


def roll(value, amount, axis):
    size = value.shape[axis]
    return pltpu.roll(value, amount % size, axis)


def time_tables(steps):
    kappa = 16.0 / (steps * steps)
    index = np.arange(steps)
    gamma = ALPHA ** (index / steps)
    lam = 1.0 - ALPHA ** (1.0 / steps) * np.exp(-2j * np.pi * index / steps)
    den = lam * lam + 4.0 * kappa
    turn = np.exp(-2j * np.pi * np.outer(index, index) / steps)
    tables = []
    for m in range(SWEEPS):
        inner = np.conj(turn) @ ((1.0 / den ** (m + 1))[:, None] * turn) / steps
        tables.append(kappa**m * (inner.real / gamma[:, None]) * gamma[None, :])
    return np.concatenate(tables, 1).astype(np.float32), kappa


def halves(value):
    high = value.astype(jnp.bfloat16)
    return high, (value - high.astype(jnp.float32)).astype(jnp.bfloat16)


def space_table():
    rows = 2 * ROWS
    shift = np.eye(rows, k=1) + np.eye(rows, k=-1)
    table = np.zeros((2, LANES, 2 * LANES))
    for m in range(SWEEPS + 1):
        for k in range(m + 1):
            part = math.comb(m, k) * np.linalg.matrix_power(shift, m - k)
            for row in range(rows):
                for out in range(rows):
                    h, at = divmod(out, ROWS)
                    lanes = [m * 4 * ROWS + h * 2 * ROWS + at]
                    if m == SWEEPS:
                        lanes = [LANES + (h * 8 + i) * ROWS + at for i in range(KRYLOV)]
                    for c in range(2):
                        source = (k * 2 + c) * ROWS + row % ROWS
                        table[row // ROWS, source, lanes] = part[row, out]
    return table.reshape(2 * LANES, 2 * LANES)


def lane_of(shape):
    return lax.broadcasted_iota(jnp.int32, shape, len(shape) - 1)


def powers_of(flat):
    cols = flat.shape[-1]
    lane = lane_of(flat.shape)
    powers = [flat]
    for _ in range(SWEEPS):
        last = powers[-1]
        right = jnp.where(lane == 0, 0.0, roll(last, 1, 1))
        left = jnp.where(lane == cols - 1, 0.0, roll(last, -1, 1))
        powers.append(right + left)
    return powers


def packed(powers, basis, lent, odd):
    half = powers[0].shape[-1] // 2
    fields = powers + [basis[i, 1] for i in range(KRYLOV)]
    fields += [jnp.where(odd, lent[i], basis[i, 0]) for i in range(2)]
    whole = jnp.concatenate(fields, 0)
    return [whole[:, dc * half : (dc + 1) * half].T for dc in range(2)]


def own_products(flat, basis):
    sums = []
    for i in range(KRYLOV):
        both = basis[i, 0] * flat[:ROWS] + basis[i, 1] * flat[ROWS:]
        sums.append(sum(both[:, at : at + LANES] for at in range(0, both.shape[1], LANES)))
    return jnp.concatenate(sums, 0)


def delayed(value):
    row = lax.broadcasted_iota(jnp.int32, value.shape, 0)
    moved = roll(value, 1, 0)
    return jnp.where(row == 0, ALPHA * moved, moved)


def dot(left, right):
    return jnp.dot(left, right, preferred_element_type=jnp.float32)


def spread_over(value, group):
    size = group
    while size < LANES:
        value = value + roll(value, size, 1)
        size *= 2
    return value


def solved(parts, own, time_high, time_low, space, kappa, count):
    steps = parts[0][0].shape[0]
    shape = (steps, LANES)
    lane = lane_of(shape)
    row = lax.broadcasted_iota(jnp.int32, shape, 0)
    is_disp = (lane & ROWS) == 0
    mixed = []
    for dc in range(2):
        sides = []
        for h in range(2):
            x = parts[h][dc]
            sides.append(jnp.where(is_disp, x - delayed(x), x))
        mixed.append(jnp.concatenate(sides, 1))
    mixed = jnp.concatenate(mixed, 0)
    high, low = halves(mixed)
    rest = (mixed - high.astype(jnp.float32) - low.astype(jnp.float32)).astype(jnp.bfloat16)
    spread = dot(high, space) + dot(low, space) + dot(rest, space)
    group = 4 * ROWS
    early = spread[:steps, :LANES] + roll(spread[steps:, :LANES], ROWS, 1)
    last = spread[:steps, LANES:] + roll(spread[steps:, LANES:], group, 1)
    stack = [jnp.where(lane // group == m, early, 0.0) for m in range(SWEEPS)]
    high, low = halves(jnp.concatenate(stack, 0))
    disp = dot(time_high, high) + (dot(time_high, low) + dot(time_low, high))
    disp = disp + roll(disp, 2 * group, 1)
    disp = disp + roll(disp, group, 1)
    high, low = halves(last)
    cut_high = time_high[:, (SWEEPS - 1) * steps :]
    cut_low = time_low[:, (SWEEPS - 1) * steps :]
    gone = dot(cut_high, high) + (dot(cut_high, low) + dot(cut_low, high))
    gone = gone * -kappa
    late = delayed(disp)
    rate = disp - late
    edge = jnp.where(row == 0, late, 0.0)
    place = (lane - OUT) // FIELD
    outs, square = [], 0.0
    for h in range(2):
        flip = lambda v, slot: roll(v, FIELD, 1) if (slot + h) % 2 else v
        add = jnp.where(place == 0, flip(disp, 0), 0.0)
        add = jnp.where(place == 1, flip(rate, 1), add)
        add = jnp.where(place == 2, flip(edge, 2), add)
        first_lane = h * 8 * ROWS + 3 * ROWS
        add = jnp.where(place == 3, roll(gone, OUT + 3 * FIELD - first_lane, 1), add)
        for dc in range(2):
            x = parts[h][dc]
            spot = (lane - OUT) // ROWS - dc
            base = OUT + dc * ROWS
            add = add - jnp.where(spot == 2, roll(x, base + FIELD, 1), 0.0)
            add = add + jnp.where(spot == 4, roll(x, base + 2 * FIELD, 1), 0.0)
            add = add + jnp.where(spot == 6, roll(x, base + 3 * FIELD - ROWS, 1), 0.0)
        wrap = jnp.where((row == 0) & (place == 3), delayed(roll(add, 2 * FIELD, 1)), 0.0)
        out = add + wrap
        outs.append(out)
        square = square + jnp.sum(jnp.where(place >= 2, out * out, 0.0), 0, keepdims=True)
    start = 10 * ROWS
    line = lane_of((1, LANES))
    where_basis = jnp.zeros(shape, jnp.float32)
    gram = jnp.zeros((1, LANES), jnp.float32)
    for h in range(2):
        ending = ALPHA * outs[h][steps - 1 :]
        for dc in range(2):
            x = parts[h][dc]
            at = (2 * h + dc) * group
            where_basis = jnp.where(lane // group == 2 * h + dc, roll(x, at - start, 1), where_basis)
            spot = (line - OUT) // ROWS - dc
            disp_row = spread_over(jnp.where(spot == 0, ending, 0.0), ROWS)
            rate_row = spread_over(jnp.where(spot == 2, ending, 0.0), ROWS)
            gram = gram + jnp.where(line < group, roll(x[:1] * rate_row, -start, 1), 0.0)
            gram = gram + jnp.where(line < FIELD, roll(x[:1] * disp_row, FIELD, 1), 0.0)
            second = (line >= FIELD) & (line < 2 * FIELD)
            gram = gram + jnp.where(second, roll(x[1:2] * disp_row, 2 * FIELD, 1), 0.0)
    product = jnp.sum(where_basis * gone, 0, keepdims=True)
    product = product + roll(product, 2 * group, 1)
    product = product + roll(product, group, 1)
    gram = gram + jnp.where(line < group, product, 0.0)
    for i in range(KRYLOV):
        total = jnp.sum(jnp.sum(own[i * ROWS : (i + 1) * ROWS], 0, keepdims=True), 1, keepdims=True)
        gram = gram + jnp.where(line == i * ROWS, total, 0.0)
    square = square + roll(square, FIELD, 1)
    square = square + roll(square, ROWS, 1)
    square = roll(square, group - (OUT + 3 * FIELD + ROWS), 1) * (1.0 / count)
    gram = jnp.where(line // ROWS == KRYLOV, square, gram)
    return [jnp.where(lane < OUT, jnp.broadcast_to(gram, shape), out) for out in outs]


def gram_of(totals):
    line = lane_of(totals.shape)
    return [jnp.sum(jnp.where(line // ROWS == i, totals, 0.0)) for i in range(KRYLOV + 1)]


def pack_kernel(resid_hbm, basis_hbm, lent_ref, send_ref, own_ref, resid_ref, basis_ref, sems):
    copies = [
        pltpu.make_async_copy(resid_hbm, resid_ref, sems.at[0]),
        pltpu.make_async_copy(basis_hbm, basis_ref, sems.at[1]),
    ]
    for copy in copies:
        copy.start()
    odd = lax.axis_index("tm") % 2 == 1
    copies[0].wait()
    flat = resid_ref[...].reshape(2 * ROWS, resid_ref.shape[-1])
    powers = powers_of(flat)
    copies[1].wait()
    basis = basis_ref[:, :, 0]
    for slot, slab in enumerate(packed(powers, basis, lent_ref[:, 0], odd)):
        send_ref[pl.ds(slot, slab.shape[0], stride=SLOTS), :] = slab
    own_ref[...] = own_products(flat, basis)


def solve_kernel(kappa, count, recv_ref, own_ref, high_ref, low_ref, space_ref, send_ref):
    steps = high_ref.shape[0]
    parts = [
        [recv_ref[pl.ds(h * SLOTS + s, steps, stride=2 * SLOTS), :] for s in range(SLOTS)]
        for h in range(2)
    ]
    tables = [own_ref[...], high_ref[...], low_ref[...], space_ref[...]]
    outs = solved(parts, *tables, kappa, count)
    for h, out in enumerate(outs):
        send_ref[pl.ds(h, steps, stride=2), :] = out


def unpack_kernel(recv_ref, precond_ref, image_ref, gram_ref):
    received = recv_ref[...]
    half = received.shape[0]
    turned = received.T
    for slot, (ref, c) in enumerate(
        ((precond_ref, 0), (precond_ref, 1), (image_ref, 0), (image_ref, 1))
    ):
        for dc in range(2):
            start = OUT + slot * FIELD + dc * ROWS
            ref[c, 0, :, dc * half : (dc + 1) * half] = turned[start : start + ROWS]
    for i, value in enumerate(gram_of(jnp.sum(received, 0, keepdims=True))):
        gram_ref[i] = value


def solution(mesh):
    axes = ("tm", "rows")
    steps = mesh.shape["tm"]
    devices = steps * mesh.shape["rows"]

    params = pltpu.CompilerParams(vmem_limit_bytes=12 * 2**20)

    def on_device(resid, basis):
        cols = resid.shape[3]
        count = 2.0 * steps * 2 * ROWS * cols
        table, kappa = time_tables(steps)
        time_high = jnp.asarray(table.astype(jnp.bfloat16))
        time_low = jnp.asarray((table - table.astype(jnp.bfloat16)).astype(jnp.bfloat16))
        space = jnp.asarray(space_table().astype(jnp.bfloat16))
        pairs = [(j, j + 1) for j in range(0, steps, 2)]
        lent = lax.ppermute(basis[2:, 0], "tm", pairs)
        vmem = pl.BlockSpec(memory_space=pltpu.VMEM)
        hbm = pl.BlockSpec(memory_space=pltpu.HBM)
        send, own = pl.pallas_call(
            pack_kernel,
            in_specs=[hbm, hbm, vmem],
            out_shape=(
                jax.ShapeDtypeStruct((devices * SLOTS, LANES), jnp.float32),
                jax.ShapeDtypeStruct((KRYLOV * ROWS, LANES), jnp.float32),
            ),
            scratch_shapes=[
                pltpu.VMEM((2, 1, ROWS, cols), jnp.float32),
                pltpu.VMEM((KRYLOV, 2, 1, ROWS, cols), jnp.float32),
                pltpu.SemaphoreType.DMA((2,)),
            ],
            compiler_params=params,
            name="pack",
        )(*(pltpu.with_memory_space_constraint(a, pltpu.HBM) for a in (resid, basis)), lent)
        send = send.reshape(devices, 1, SLOTS * LANES)
        recv = lax.all_to_all(send, axes, 0, 0, tiled=True)
        recv = recv.reshape(devices * SLOTS, LANES)
        back = pl.pallas_call(
            lambda *refs: solve_kernel(kappa, count, *refs),
            out_shape=jax.ShapeDtypeStruct((devices, LANES), jnp.float32),
            compiler_params=params,
            name="solve",
        )(recv, own, time_high, time_low, space)
        home = lax.all_to_all(back, axes, 0, 0, tiled=True)
        shard = jax.ShapeDtypeStruct(resid.shape, jnp.float32)
        precond, image, gram = pl.pallas_call(
            unpack_kernel,
            out_shape=(shard, shard, jax.ShapeDtypeStruct((KRYLOV + 1,), jnp.float32)),
            out_specs=(vmem, vmem, pl.BlockSpec(memory_space=pltpu.SMEM)),
            compiler_params=params,
            name="unpack",
        )(home)
        return precond, image, gram

    return jax.shard_map(
        on_device,
        mesh=mesh,
        in_specs=(P(None, "tm", "rows", None), P(None, None, "tm", "rows", None)),
        out_specs=(P(None, "tm", "rows", None), P(None, "tm", "rows", None), P()),
        check_vma=False,
    )
```

```python
import math

import jax
import jax.numpy as jnp
import numpy as np
from jax import lax
from jax.experimental import pallas as pl
from jax.experimental.pallas import tpu as pltpu
from jax.sharding import PartitionSpec as P

ALPHA = 0.01
SWEEPS = 4
KRYLOV = 4
LANES = 128
ROWS = 8
SLOTS = 2
FIELD = 2 * ROWS
OUT = 64


def roll(value, amount, axis):
    size = value.shape[axis]
    return pltpu.roll(value, amount % size, axis)


def time_tables(steps):
    kappa = 16.0 / (steps * steps)
    index = np.arange(steps)
    gamma = ALPHA ** (index / steps)
    lam = 1.0 - ALPHA ** (1.0 / steps) * np.exp(-2j * np.pi * index / steps)
    den = lam * lam + 4.0 * kappa
    turn = np.exp(-2j * np.pi * np.outer(index, index) / steps)
    tables = []
    for m in range(SWEEPS):
        inner = np.conj(turn) @ ((1.0 / den ** (m + 1))[:, None] * turn) / steps
        tables.append(kappa**m * (inner.real / gamma[:, None]) * gamma[None, :])
    return np.concatenate(tables, 1).astype(np.float32), kappa


def halves(value):
    high = value.astype(jnp.bfloat16)
    return high, (value - high.astype(jnp.float32)).astype(jnp.bfloat16)


def space_table():
    rows = 2 * ROWS
    shift = np.eye(rows, k=1) + np.eye(rows, k=-1)
    table = np.zeros((2, LANES, 2 * LANES))
    for m in range(SWEEPS + 1):
        for k in range(m + 1):
            part = math.comb(m, k) * np.linalg.matrix_power(shift, m - k)
            for row in range(rows):
                for out in range(rows):
                    h, at = divmod(out, ROWS)
                    lanes = [m * 4 * ROWS + h * 2 * ROWS + at]
                    if m == SWEEPS:
                        lanes = [LANES + (h * 8 + i) * ROWS + at for i in range(KRYLOV)]
                    for c in range(2):
                        source = (k * 2 + c) * ROWS + row % ROWS
                        table[row // ROWS, source, lanes] = part[row, out]
    return table.reshape(2 * LANES, 2 * LANES)


def lane_of(shape):
    return lax.broadcasted_iota(jnp.int32, shape, len(shape) - 1)


def powers_of(flat):
    cols = flat.shape[-1]
    lane = lane_of(flat.shape)
    powers = [flat]
    for _ in range(SWEEPS):
        last = powers[-1]
        right = jnp.where(lane == 0, 0.0, roll(last, 1, 1))
        left = jnp.where(lane == cols - 1, 0.0, roll(last, -1, 1))
        powers.append(right + left)
    return powers


def packed(powers, basis, lent, odd):
    half = powers[0].shape[-1] // 2
    fields = powers + [basis[i, 1] for i in range(KRYLOV)]
    fields += [jnp.where(odd, lent[i], basis[i, 0]) for i in range(2)]
    whole = jnp.concatenate(fields, 0)
    return [whole[:, dc * half : (dc + 1) * half].T for dc in range(2)]


def own_products(flat, basis):
    sums = []
    for i in range(KRYLOV):
        both = basis[i, 0] * flat[:ROWS] + basis[i, 1] * flat[ROWS:]
        sums.append(sum(both[:, at : at + LANES] for at in range(0, both.shape[1], LANES)))
    return jnp.concatenate(sums, 0)


def delayed(value):
    row = lax.broadcasted_iota(jnp.int32, value.shape, 0)
    moved = roll(value, 1, 0)
    return jnp.where(row == 0, ALPHA * moved, moved)


def dot(left, right):
    return jnp.dot(left, right, preferred_element_type=jnp.float32)


def spread_over(value, group):
    size = group
    while size < LANES:
        value = value + roll(value, size, 1)
        size *= 2
    return value


def solved(parts, own, time_high, time_low, space, kappa, count):
    steps = parts[0][0].shape[0]
    shape = (steps, LANES)
    lane = lane_of(shape)
    row = lax.broadcasted_iota(jnp.int32, shape, 0)
    is_disp = (lane & ROWS) == 0
    mixed = []
    for dc in range(2):
        sides = []
        for h in range(2):
            x = parts[h][dc]
            sides.append(jnp.where(is_disp, x - delayed(x), x))
        mixed.append(jnp.concatenate(sides, 1))
    mixed = jnp.concatenate(mixed, 0)
    high, low = halves(mixed)
    rest = (mixed - high.astype(jnp.float32) - low.astype(jnp.float32)).astype(jnp.bfloat16)
    spread = dot(high, space) + dot(low, space) + dot(rest, space)
    group = 4 * ROWS
    early = spread[:steps, :LANES] + roll(spread[steps:, :LANES], ROWS, 1)
    last = spread[:steps, LANES:] + roll(spread[steps:, LANES:], group, 1)
    stack = [jnp.where(lane // group == m, early, 0.0) for m in range(SWEEPS)]
    high, low = halves(jnp.concatenate(stack, 0))
    disp = dot(time_high, high) + (dot(time_high, low) + dot(time_low, high))
    disp = disp + roll(disp, 2 * group, 1)
    disp = disp + roll(disp, group, 1)
    high, low = halves(last)
    cut_high = time_high[:, (SWEEPS - 1) * steps :]
    cut_low = time_low[:, (SWEEPS - 1) * steps :]
    gone = dot(cut_high, high) + (dot(cut_high, low) + dot(cut_low, high))
    gone = gone * -kappa
    late = delayed(disp)
    rate = disp - late
    edge = jnp.where(row == 0, late, 0.0)
    place = (lane - OUT) // FIELD
    outs, square = [], 0.0
    for h in range(2):
        flip = lambda v, slot: roll(v, FIELD, 1) if (slot + h) % 2 else v
        add = jnp.where(place == 0, flip(disp, 0), 0.0)
        add = jnp.where(place == 1, flip(rate, 1), add)
        add = jnp.where(place == 2, flip(edge, 2), add)
        first_lane = h * 8 * ROWS + 3 * ROWS
        add = jnp.where(place == 3, roll(gone, OUT + 3 * FIELD - first_lane, 1), add)
        for dc in range(2):
            x = parts[h][dc]
            spot = (lane - OUT) // ROWS - dc
            base = OUT + dc * ROWS
            add = add - jnp.where(spot == 2, roll(x, base + FIELD, 1), 0.0)
            add = add + jnp.where(spot == 4, roll(x, base + 2 * FIELD, 1), 0.0)
            add = add + jnp.where(spot == 6, roll(x, base + 3 * FIELD - ROWS, 1), 0.0)
        wrap = jnp.where((row == 0) & (place == 3), delayed(roll(add, 2 * FIELD, 1)), 0.0)
        out = add + wrap
        outs.append(out)
        square = square + jnp.sum(jnp.where(place >= 2, out * out, 0.0), 0, keepdims=True)
    start = 10 * ROWS
    line = lane_of((1, LANES))
    where_basis = jnp.zeros(shape, jnp.float32)
    gram = jnp.zeros((1, LANES), jnp.float32)
    for h in range(2):
        ending = ALPHA * outs[h][steps - 1 :]
        for dc in range(2):
            x = parts[h][dc]
            at = (2 * h + dc) * group
            where_basis = jnp.where(lane // group == 2 * h + dc, roll(x, at - start, 1), where_basis)
            spot = (line - OUT) // ROWS - dc
            disp_row = spread_over(jnp.where(spot == 0, ending, 0.0), ROWS)
            rate_row = spread_over(jnp.where(spot == 2, ending, 0.0), ROWS)
            gram = gram + jnp.where(line < group, roll(x[:1] * rate_row, -start, 1), 0.0)
            gram = gram + jnp.where(line < FIELD, roll(x[:1] * disp_row, FIELD, 1), 0.0)
            second = (line >= FIELD) & (line < 2 * FIELD)
            gram = gram + jnp.where(second, roll(x[1:2] * disp_row, 2 * FIELD, 1), 0.0)
    product = jnp.sum(where_basis * gone, 0, keepdims=True)
    product = product + roll(product, 2 * group, 1)
    product = product + roll(product, group, 1)
    gram = gram + jnp.where(line < group, product, 0.0)
    for i in range(KRYLOV):
        total = jnp.sum(jnp.sum(own[i * ROWS : (i + 1) * ROWS], 0, keepdims=True), 1, keepdims=True)
        gram = gram + jnp.where(line == i * ROWS, total, 0.0)
    square = square + roll(square, FIELD, 1)
    square = square + roll(square, ROWS, 1)
    square = roll(square, group - (OUT + 3 * FIELD + ROWS), 1) * (1.0 / count)
    gram = jnp.where(line // ROWS == KRYLOV, square, gram)
    return [jnp.where(lane < OUT, jnp.broadcast_to(gram, shape), out) for out in outs]


def gram_of(totals):
    line = lane_of(totals.shape)
    return [jnp.sum(jnp.where(line // ROWS == i, totals, 0.0)) for i in range(KRYLOV + 1)]


def pack_kernel(resid_hbm, basis_hbm, lent_ref, send_ref, own_ref, resid_ref, basis_ref, sems):
    copies = [
        pltpu.make_async_copy(resid_hbm, resid_ref, sems.at[0]),
        pltpu.make_async_copy(basis_hbm, basis_ref, sems.at[1]),
    ]
    for copy in copies:
        copy.start()
    odd = lax.axis_index("tm") == 1
    copies[0].wait()
    flat = resid_ref[...].reshape(2 * ROWS, resid_ref.shape[-1])
    powers = powers_of(flat)
    copies[1].wait()
    basis = basis_ref[:, :, 0]
    for slot, slab in enumerate(packed(powers, basis, lent_ref[2:, 0, 0], odd)):
        send_ref[pl.ds(slot, slab.shape[0], stride=SLOTS), :] = slab
    own_ref[...] = own_products(flat, basis)


def solve_kernel(kappa, count, recv_ref, own_ref, high_ref, low_ref, space_ref, send_ref):
    steps = high_ref.shape[0]
    parts = [
        [recv_ref[pl.ds(h * SLOTS + s, steps, stride=2 * SLOTS), :] for s in range(SLOTS)]
        for h in range(2)
    ]
    tables = [own_ref[...], high_ref[...], low_ref[...], space_ref[...]]
    outs = solved(parts, *tables, kappa, count)
    for h, out in enumerate(outs):
        send_ref[pl.ds(h, steps, stride=2), :] = out


def unpack_kernel(recv_ref, precond_ref, image_ref, gram_ref):
    received = recv_ref[...]
    half = received.shape[0]
    turned = received.T
    for slot, (ref, c) in enumerate(
        ((precond_ref, 0), (precond_ref, 1), (image_ref, 0), (image_ref, 1))
    ):
        for dc in range(2):
            start = OUT + slot * FIELD + dc * ROWS
            ref[c, 0, :, dc * half : (dc + 1) * half] = turned[start : start + ROWS]
    for i, value in enumerate(gram_of(jnp.sum(received, 0, keepdims=True))):
        gram_ref[i] = value


def solution(mesh):
    axes = ("tm", "rows")
    steps = mesh.shape["tm"]
    devices = steps * mesh.shape["rows"]

    params = pltpu.CompilerParams(vmem_limit_bytes=12 * 2**20)

    def on_device(resid, basis):
        cols = resid.shape[3]
        count = 2.0 * steps * 2 * ROWS * cols
        table, kappa = time_tables(steps)
        time_high = jnp.asarray(table.astype(jnp.bfloat16))
        time_low = jnp.asarray((table - table.astype(jnp.bfloat16)).astype(jnp.bfloat16))
        space = jnp.asarray(space_table().astype(jnp.bfloat16))
        lent = lax.ppermute(basis, "tm", [(0, 1)])
        vmem = pl.BlockSpec(memory_space=pltpu.VMEM)
        hbm = pl.BlockSpec(memory_space=pltpu.HBM)
        send, own = pl.pallas_call(
            pack_kernel,
            in_specs=[hbm, hbm, vmem],
            out_shape=(
                jax.ShapeDtypeStruct((devices * SLOTS, LANES), jnp.float32),
                jax.ShapeDtypeStruct((KRYLOV * ROWS, LANES), jnp.float32),
            ),
            scratch_shapes=[
                pltpu.VMEM((2, 1, ROWS, cols), jnp.float32),
                pltpu.VMEM((KRYLOV, 2, 1, ROWS, cols), jnp.float32),
                pltpu.SemaphoreType.DMA((2,)),
            ],
            compiler_params=params,
            name="pack",
        )(*(pltpu.with_memory_space_constraint(a, pltpu.HBM) for a in (resid, basis)), lent)
        send = send.reshape(devices, 1, SLOTS * LANES)
        recv = lax.all_to_all(send, axes, 0, 0, tiled=True)
        recv = recv.reshape(devices * SLOTS, LANES)
        back = pl.pallas_call(
            lambda *refs: solve_kernel(kappa, count, *refs),
            out_shape=jax.ShapeDtypeStruct((devices, LANES), jnp.float32),
            compiler_params=params,
            name="solve",
        )(recv, own, time_high, time_low, space)
        home = lax.all_to_all(back, axes, 0, 0, tiled=True)
        shard = jax.ShapeDtypeStruct(resid.shape, jnp.float32)
        precond, image, gram = pl.pallas_call(
            unpack_kernel,
            out_shape=(shard, shard, jax.ShapeDtypeStruct((KRYLOV + 1,), jnp.float32)),
            out_specs=(vmem, vmem, pl.BlockSpec(memory_space=pltpu.SMEM)),
            compiler_params=params,
            name="unpack",
        )(home)
        return precond, image, gram

    return jax.shard_map(
        on_device,
        mesh=mesh,
        in_specs=(P(None, "tm", "rows", None), P(None, None, "tm", "rows", None)),
        out_specs=(P(None, "tm", "rows", None), P(None, "tm", "rows", None), P()),
        check_vma=False,
    )
```

```python
import jax
import jax.numpy as jnp
import numpy as np
from jax import lax
from jax.experimental import pallas as pl
from jax.experimental.pallas import tpu as pltpu
from jax.sharding import PartitionSpec as P

ALPHA = 0.01
SWEEPS = 4
KRYLOV = 4
LANES = 128
ROWS = 8
SIDE = LANES // 2
MODES = 2 * ROWS
GROUP = 2 * MODES


def roll(value, amount, axis):
    size = value.shape[axis]
    return pltpu.roll(value, amount % size, axis)


def reversed_lanes(value):
    parts = [value[:, at : at + LANES] for at in range(0, value.shape[1], LANES)]
    index = LANES - 1 - lane_of(parts[0].shape)
    taken = [jnp.take_along_axis(p, index, axis=1, mode="promise_in_bounds") for p in parts]
    return jnp.concatenate(taken[::-1], 1)


def lane_of(shape):
    return lax.broadcasted_iota(jnp.int32, shape, len(shape) - 1)


def row_of(shape):
    return lax.broadcasted_iota(jnp.int32, shape, 0)


def sines(number, place, length):
    turn = np.outer(number, place + 1.0) / (length + 1)
    return np.sqrt(2.0 / (length + 1)) * np.sin(np.pi * turn)


def coupling(steps):
    return 16.0 / (steps * steps)


def time_table(steps):
    kappa = coupling(steps)
    index = np.arange(steps)
    gamma = ALPHA ** (index / steps)
    lam = 1.0 - ALPHA ** (1.0 / steps) * np.exp(-2j * np.pi * index / steps)
    den = lam * lam + 4.0 * kappa
    turn = np.exp(-2j * np.pi * np.outer(index, index) / steps)
    tables = []
    for m in range(SWEEPS):
        inner = np.conj(turn) @ ((1.0 / den ** (m + 1))[:, None] * turn) / steps
        tables.append(kappa**m * (inner.real / gamma[:, None]) * gamma[None, :])
    return np.concatenate(tables, 1)


def column_numbers(cols):
    return [2.0 * np.arange(cols // 2) + 1 + dc for dc in range(2)]


def column_tables(cols):
    return np.stack([sines(n, np.arange(cols // 2), cols) for n in column_numbers(cols)])


def symbol_table(cols):
    rows = 2.0 * np.cos(np.pi * (np.arange(MODES) + 1) / (MODES + 1))
    sums = []
    for number in column_numbers(cols):
        sums.append(2.0 * np.cos(np.pi * number / (cols + 1))[:, None] + rows[None, :])
    return np.tile(np.concatenate(sums, 1), (1, LANES // GROUP)).astype(np.float32)


def row_tables():
    wave = sines(np.arange(MODES) + 1, np.arange(MODES), MODES)
    enter = np.zeros((2, LANES, LANES))
    leave = np.zeros((LANES, 2, 2, LANES))
    for h in range(2):
        for row in range(ROWS):
            for dc in range(2):
                value = wave[:, h * ROWS + row]
                modes = dc * MODES + np.arange(MODES)
                for group in range(0, LANES, GROUP):
                    for c in range(2):
                        enter[h, dc * SIDE + c * ROWS + row, group + modes] = value
                for field, group in enumerate((0, 2, 1, 3)):
                    leave[group * GROUP + modes, 0, h, dc * SIDE + field * ROWS + row] = value
                for slot in range(1, 2 + KRYLOV):
                    leave[GROUP + modes, 1, h, dc * SIDE + slot * ROWS + row] = value
    return enter.reshape(2 * LANES, LANES), leave.reshape(LANES, 4 * LANES)


def halves(value):
    high = value.astype(jnp.bfloat16)
    return high, (value - high.astype(jnp.float32)).astype(jnp.bfloat16)


def both_halves(table):
    high = table.astype(jnp.bfloat16)
    return jnp.asarray(np.stack([high, (table - high.astype(np.float64)).astype(jnp.bfloat16)]))


def product(left, right, contract=((1,), (0,))):
    total = 0.0
    for i, j in ((1, 0), (0, 1), (0, 0)):
        total = total + lax.dot_general(
            left[i], right[j], (contract, ((), ())), preferred_element_type=jnp.float32
        )
    return total


def packed(flat, basis, lent, second, tables):
    half = flat.shape[1] // 2
    fields = [flat] + [basis[i, 1] for i in range(KRYLOV)]
    fields += [jnp.where(second, lent[i], basis[i, 0]) for i in range(2)]
    whole = jnp.concatenate(fields, 0)
    left, right = whole[:, :half], reversed_lanes(whole[:, half:])
    sides = []
    for dc, folded in enumerate((left + right, left - right)):
        table = (tables[0, dc], tables[1, dc])
        sides.append(product(table, halves(folded), ((1,), (1,))))
    return jnp.concatenate(sides, 1)


def own_products(flat, basis):
    disp, velo = flat[:ROWS], flat[ROWS:]
    terms = [basis[i, 0] * disp + basis[i, 1] * velo for i in range(KRYLOV)]
    terms.append(disp * disp + velo * velo)
    sums = [sum(t[:, at : at + LANES] for at in range(0, t.shape[1], LANES)) for t in terms]
    return jnp.concatenate(sums, 0)


def delayed(value):
    moved = roll(value, 1, 0)
    return jnp.where(row_of(value.shape) == 0, ALPHA * moved, moved)


def solved(parts, own, symbol, time, enter, leave, kappa, count):
    steps = parts[0].shape[0]
    shape = (steps, LANES)
    lane, row = lane_of(shape), row_of(shape)
    is_disp = lane % SIDE < ROWS
    mixed = [jnp.where(is_disp, x - delayed(x), x) for x in parts]
    source = product(halves(jnp.concatenate(mixed, 1)), enter)
    line = lane_of((1, LANES))
    cut = line // GROUP == 1
    power, weights = jnp.ones((1, LANES), jnp.float32), []
    for m in range(SWEEPS):
        last = -kappa * power * symbol if m == SWEEPS - 1 else 0.0
        weights.append(jnp.where(cut, last, power))
        power = power * symbol
    stack = jnp.concatenate([source * weight for weight in weights], 0)
    found = product(time, halves(stack))
    late = delayed(found)
    group = lane // GROUP
    found = jnp.where(group == 2, found - late, found)
    found = jnp.where(group == 3, jnp.where(row == 0, late, 0.0), found)
    spread = product(halves(found), leave)
    at = line % SIDE
    slot = at // ROWS
    outs, gram, square = [], 0.0, 0.0
    for h, x in enumerate(parts):
        out = spread[:, h * LANES : (h + 1) * LANES]
        gone = spread[:, (2 + h) * LANES : (3 + h) * LANES]
        ended = roll(out[steps - 1 :], ROWS, 1) - roll(x[steps - 1 :], 2 * ROWS, 1)
        rate = jnp.where(slot == 2, ALPHA * ended, 0.0)
        outs.append(jnp.where((row == 0) & (slot == 2), out + rate, out))
        disp = jnp.where(slot == 3, out[:1], 0.0)
        inner = jnp.sum(jnp.where(slot[:1] >= 2, x * gone, gone * (2.0 * x + gone)), 0, keepdims=True)
        wide = rate + roll(rate, ROWS, 1)
        wide = wide + roll(wide, 2 * ROWS, 1)
        tail = roll(disp, 3 * ROWS, 1)
        tail = tail + roll(tail, ROWS, 1)
        gram = gram + jnp.where((slot >= 2) & (slot < 2 + KRYLOV), inner + x[:1] * wide, 0.0)
        gram = gram + jnp.where((slot == 2) | (slot == 3), roll(x[:1] * tail, -4 * ROWS, 1), 0.0)
        gram = gram + jnp.where((slot == 4) | (slot == 5), roll(x[1:2] * tail, -2 * ROWS, 1), 0.0)
        rate, disp = roll(rate, -ROWS, 1), roll(disp, -3 * ROWS, 1)
        square = square + jnp.where(slot == 1, inner + rate * (2.0 * (x[:1] + gone[:1]) + rate), 0.0)
        square = square + jnp.where(slot == 0, disp * (2.0 * x[:1] + disp), 0.0)
    totals = [
        jnp.sum(jnp.sum(own[i * ROWS : (i + 1) * ROWS], 0, keepdims=True), 1, keepdims=True)
        for i in range(KRYLOV + 1)
    ]
    gram = gram + roll(gram, SIDE, 1)
    for i in range(KRYLOV):
        gram = gram + jnp.where(line == (2 + i) * ROWS, totals[i], 0.0)
    square = square + roll(square, SIDE, 1)
    square = square + roll(square, ROWS, 1)
    square = (square + jnp.where(line == SIDE + ROWS, totals[KRYLOV], 0.0)) * (1.0 / count)
    gram = roll(gram, GROUP - 2 * ROWS, 1)
    square = roll(square, GROUP - ROWS, 1)
    gram = jnp.where(line < SIDE, gram, square)
    return [jnp.where(lane % SIDE >= GROUP, jnp.broadcast_to(gram, shape), out) for out in outs]


def gram_of(totals):
    place = lane_of(totals.shape) // ROWS
    wanted = [GROUP // ROWS + i for i in range(KRYLOV)] + [(SIDE + GROUP) // ROWS]
    return [jnp.sum(jnp.where(place == at, totals, 0.0)) for at in wanted]


def unpacked(received, flat, tables):
    turned = received.T
    sides = []
    for dc in range(2):
        fields = turned[dc * SIDE : dc * SIDE + GROUP]
        sides.append(product(halves(fields), (tables[0, dc], tables[1, dc])))
    whole = jnp.concatenate([sides[0] + sides[1], reversed_lanes(sides[0] - sides[1])], 1)
    disp, rate, cut, edge = [whole[i * ROWS : (i + 1) * ROWS] for i in range(4)]
    return disp, rate - flat[:ROWS], flat[:ROWS] + edge, flat[ROWS:] + cut


def pack_kernel(
    resid_hbm, basis_hbm, tables_hbm, lent_ref, send_ref, own_ref, resid_ref, basis_ref, tables_ref, sems
):
    pairs = ((resid_hbm, resid_ref), (basis_hbm, basis_ref), (tables_hbm, tables_ref))
    copies = [pltpu.make_async_copy(a, b, sems.at[i]) for i, (a, b) in enumerate(pairs)]
    for copy in copies:
        copy.start()
    second = lax.axis_index("tm") == 1
    for copy in copies:
        copy.wait()
    flat = resid_ref[...].reshape(MODES, resid_ref.shape[-1])
    basis = basis_ref[:, :, 0]
    send_ref[...] = packed(flat, basis, lent_ref[2:, 0, 0], second, tables_ref)
    own_ref[...] = own_products(flat, basis)


def solve_kernel(
    kappa, count, recv_ref, own_ref, symbol_ref, time_ref, enter_ref, leave_ref, send_ref
):
    steps = time_ref.shape[1]
    here = lax.axis_index("tm") * 2 + lax.axis_index("rows")
    parts = [recv_ref[pl.ds(h, steps, stride=2), :] for h in range(2)]
    outs = solved(
        parts, own_ref[...], symbol_ref[pl.ds(here, 1), :], time_ref, enter_ref, leave_ref, kappa, count
    )
    for h, out in enumerate(outs):
        send_ref[pl.ds(h, steps, stride=2), :] = out


def unpack_kernel(recv_ref, resid_ref, tables_ref, precond_ref, image_ref, gram_ref):
    received = recv_ref[...]
    flat = resid_ref[...].reshape(MODES, resid_ref.shape[-1])
    fields = unpacked(received, flat, tables_ref)
    for slot, field in enumerate(fields):
        (precond_ref, image_ref)[slot // 2][slot % 2, 0] = field
    for i, value in enumerate(gram_of(jnp.sum(received, 0, keepdims=True))):
        gram_ref[i] = value


def solution(mesh):
    axes = ("tm", "rows")
    steps = mesh.shape["tm"]
    devices = steps * mesh.shape["rows"]
    params = pltpu.CompilerParams(vmem_limit_bytes=12 * 2**20)

    def on_device(resid, basis):
        cols = resid.shape[3]
        kappa = coupling(steps)
        count = 2.0 * steps * MODES * cols
        tables = both_halves(column_tables(cols))
        enter, leave = (both_halves(t) for t in row_tables())
        lent = lax.ppermute(basis, "tm", [(0, 1)])
        vmem = pl.BlockSpec(memory_space=pltpu.VMEM)
        hbm = pl.BlockSpec(memory_space=pltpu.HBM)
        fixed = [pltpu.with_memory_space_constraint(a, pltpu.HBM) for a in (resid, basis, tables)]
        message = jax.ShapeDtypeStruct((devices, LANES), jnp.float32)
        send, own = pl.pallas_call(
            pack_kernel,
            in_specs=[hbm, hbm, hbm, vmem],
            out_shape=(message, jax.ShapeDtypeStruct(((KRYLOV + 1) * ROWS, LANES), jnp.float32)),
            scratch_shapes=[
                pltpu.VMEM(resid.shape, jnp.float32),
                pltpu.VMEM(basis.shape, jnp.float32),
                pltpu.VMEM(tables.shape, jnp.bfloat16),
                pltpu.SemaphoreType.DMA((3,)),
            ],
            compiler_params=params,
            name="pack",
        )(*fixed, lent)
        recv = lax.all_to_all(send, axes, 0, 0, tiled=True)
        back = pl.pallas_call(
            lambda *refs: solve_kernel(kappa, count, *refs),
            out_shape=message,
            compiler_params=params,
            name="solve",
        )(recv, own, jnp.asarray(symbol_table(cols)), both_halves(time_table(steps)), enter, leave)
        home = lax.all_to_all(back, axes, 0, 0, tiled=True)
        shard = jax.ShapeDtypeStruct(resid.shape, jnp.float32)
        precond, image, gram = pl.pallas_call(
            unpack_kernel,
            out_shape=(shard, shard, jax.ShapeDtypeStruct((KRYLOV + 1,), jnp.float32)),
            out_specs=(vmem, vmem, pl.BlockSpec(memory_space=pltpu.SMEM)),
            compiler_params=params,
            name="unpack",
        )(home, resid, tables)
        return precond, image, gram

    return jax.shard_map(
        on_device,
        mesh=mesh,
        in_specs=(P(None, "tm", "rows", None), P(None, None, "tm", "rows", None)),
        out_specs=(P(None, "tm", "rows", None), P(None, "tm", "rows", None), P()),
        check_vma=False,
    )
```

```python
import jax
import jax.numpy as jnp
import numpy as np
from jax import lax
from jax.experimental import pallas as pl
from jax.experimental.pallas import tpu as pltpu
from jax.sharding import PartitionSpec as P

ALPHA = 0.01
SWEEPS = 4
KRYLOV = 4
LANES = 128
ROWS = 8
SIDE = LANES // 2
MODES = 2 * ROWS
GROUP = 2 * MODES


def roll(value, amount, axis):
    size = value.shape[axis]
    return pltpu.roll(value, amount % size, axis)


def reversed_lanes(value):
    parts = [value[:, at : at + LANES] for at in range(0, value.shape[1], LANES)]
    index = LANES - 1 - lane_of(parts[0].shape)
    taken = [jnp.take_along_axis(p, index, axis=1, mode="promise_in_bounds") for p in parts]
    return jnp.concatenate(taken[::-1], 1)


def lane_of(shape):
    return lax.broadcasted_iota(jnp.int32, shape, len(shape) - 1)


def row_of(shape):
    return lax.broadcasted_iota(jnp.int32, shape, 0)


def sines(number, place, length):
    turn = np.outer(number, place + 1.0) / (length + 1)
    return np.sqrt(2.0 / (length + 1)) * np.sin(np.pi * turn)


def coupling(steps):
    return 16.0 / (steps * steps)


def time_table(steps):
    kappa = coupling(steps)
    index = np.arange(steps)
    gamma = ALPHA ** (index / steps)
    lam = 1.0 - ALPHA ** (1.0 / steps) * np.exp(-2j * np.pi * index / steps)
    den = lam * lam + 4.0 * kappa
    turn = np.exp(-2j * np.pi * np.outer(index, index) / steps)
    tables = []
    for m in range(SWEEPS):
        inner = np.conj(turn) @ ((1.0 / den ** (m + 1))[:, None] * turn) / steps
        tables.append(kappa**m * (inner.real / gamma[:, None]) * gamma[None, :])
    return np.concatenate(tables, 1)


def column_numbers(cols):
    return [2.0 * np.arange(cols // 2) + 1 + dc for dc in range(2)]


def column_tables(cols):
    return np.stack([sines(n, np.arange(cols // 2), cols) for n in column_numbers(cols)])


def symbol_table(cols):
    rows = 2.0 * np.cos(np.pi * (np.arange(MODES) + 1) / (MODES + 1))
    sums = []
    for number in column_numbers(cols):
        sums.append(2.0 * np.cos(np.pi * number / (cols + 1))[:, None] + rows[None, :])
    return np.tile(np.concatenate(sums, 1), (1, LANES // GROUP)).astype(np.float32)


def row_tables():
    wave = sines(np.arange(MODES) + 1, np.arange(MODES), MODES)
    enter = np.zeros((2, LANES, LANES))
    leave = np.zeros((LANES, 2, 2, LANES))
    for h in range(2):
        for row in range(ROWS):
            for dc in range(2):
                value = wave[:, h * ROWS + row]
                modes = dc * MODES + np.arange(MODES)
                for group in range(0, LANES, GROUP):
                    for c in range(2):
                        enter[h, dc * SIDE + c * ROWS + row, group + modes] = value
                for field, group in enumerate((0, 2, 1, 3)):
                    leave[group * GROUP + modes, 0, h, dc * SIDE + field * ROWS + row] = value
                for slot in range(1, 2 + KRYLOV):
                    leave[GROUP + modes, 1, h, dc * SIDE + slot * ROWS + row] = value
    return enter.reshape(2 * LANES, LANES), leave.reshape(LANES, 4 * LANES)


def halves(value):
    high = value.astype(jnp.bfloat16)
    return high, (value - high.astype(jnp.float32)).astype(jnp.bfloat16)


def both_halves(table):
    high = table.astype(jnp.bfloat16)
    return jnp.asarray(np.stack([high, (table - high.astype(np.float64)).astype(jnp.bfloat16)]))


def product(left, right, contract=((1,), (0,))):
    total = 0.0
    for i, j in ((1, 0), (0, 1), (0, 0)):
        total = total + lax.dot_general(
            left[i], right[j], (contract, ((), ())), preferred_element_type=jnp.float32
        )
    return total


def packed(fields, lent, second, tables):
    half = fields.shape[1] // 2
    kept = fields.shape[0] - lent.shape[0]
    whole = jnp.concatenate([fields[:kept], jnp.where(second, lent, fields[kept:])], 0)
    left, right = whole[:, :half], reversed_lanes(whole[:, half:])
    sides = []
    for dc, folded in enumerate((left + right, left - right)):
        table = (tables[0, dc], tables[1, dc])
        sides.append(product(table, halves(folded), ((1,), (1,))))
    return jnp.concatenate(sides, 1)


def own_products(fields, given):
    rows = [fields[at : at + ROWS] for at in range(0, fields.shape[0], ROWS)]
    rows += [given[at : at + ROWS] for at in range(0, given.shape[0], ROWS)]
    disp, velo, rest = rows[0], rows[1], rows[2:]
    terms = [rest[KRYLOV + i] * disp + rest[i] * velo for i in range(KRYLOV)]
    terms.append(disp * disp + velo * velo)
    sums = [sum(t[:, at : at + LANES] for at in range(0, t.shape[1], LANES)) for t in terms]
    return jnp.concatenate(sums, 0)


def delayed(value):
    moved = roll(value, 1, 0)
    return jnp.where(row_of(value.shape) == 0, ALPHA * moved, moved)


def solved(parts, own, symbol, time, enter, leave, kappa, count):
    steps = parts[0].shape[0]
    shape = (steps, LANES)
    lane, row = lane_of(shape), row_of(shape)
    is_disp = lane % SIDE < ROWS
    mixed = [jnp.where(is_disp, x - delayed(x), x) for x in parts]
    source = product(halves(jnp.concatenate(mixed, 1)), enter)
    line = lane_of((1, LANES))
    cut = line // GROUP == 1
    power, weights = jnp.ones((1, LANES), jnp.float32), []
    for m in range(SWEEPS):
        last = -kappa * power * symbol if m == SWEEPS - 1 else 0.0
        weights.append(jnp.where(cut, last, power))
        power = power * symbol
    stack = jnp.concatenate([source * weight for weight in weights], 0)
    found = product(time, halves(stack))
    late = delayed(found)
    group = lane // GROUP
    found = jnp.where(group == 2, found - late, found)
    found = jnp.where(group == 3, jnp.where(row == 0, late, 0.0), found)
    spread = product(halves(found), leave)
    at = line % SIDE
    slot = at // ROWS
    outs, gram, square = [], 0.0, 0.0
    for h, x in enumerate(parts):
        out = spread[:, h * LANES : (h + 1) * LANES]
        gone = spread[:, (2 + h) * LANES : (3 + h) * LANES]
        ended = roll(out[steps - 1 :], ROWS, 1) - roll(x[steps - 1 :], 2 * ROWS, 1)
        rate = jnp.where(slot == 2, ALPHA * ended, 0.0)
        outs.append(jnp.where((row == 0) & (slot == 2), out + rate, out))
        disp = jnp.where(slot == 3, out[:1], 0.0)
        inner = jnp.sum(jnp.where(slot[:1] >= 2, x * gone, gone * (2.0 * x + gone)), 0, keepdims=True)
        wide = rate + roll(rate, ROWS, 1)
        wide = wide + roll(wide, 2 * ROWS, 1)
        tail = roll(disp, 3 * ROWS, 1)
        tail = tail + roll(tail, ROWS, 1)
        gram = gram + jnp.where((slot >= 2) & (slot < 2 + KRYLOV), inner + x[:1] * wide, 0.0)
        gram = gram + jnp.where((slot == 2) | (slot == 3), roll(x[:1] * tail, -4 * ROWS, 1), 0.0)
        gram = gram + jnp.where((slot == 4) | (slot == 5), roll(x[1:2] * tail, -2 * ROWS, 1), 0.0)
        rate, disp = roll(rate, -ROWS, 1), roll(disp, -3 * ROWS, 1)
        square = square + jnp.where(slot == 1, inner + rate * (2.0 * (x[:1] + gone[:1]) + rate), 0.0)
        square = square + jnp.where(slot == 0, disp * (2.0 * x[:1] + disp), 0.0)
    totals = [
        jnp.sum(jnp.sum(own[i * ROWS : (i + 1) * ROWS], 0, keepdims=True), 1, keepdims=True)
        for i in range(KRYLOV + 1)
    ]
    gram = gram + roll(gram, SIDE, 1)
    for i in range(KRYLOV):
        gram = gram + jnp.where(line == (2 + i) * ROWS, totals[i], 0.0)
    square = square + roll(square, SIDE, 1)
    square = square + roll(square, ROWS, 1)
    square = (square + jnp.where(line == SIDE + ROWS, totals[KRYLOV], 0.0)) * (1.0 / count)
    gram = roll(gram, GROUP - 2 * ROWS, 1)
    square = roll(square, GROUP - ROWS, 1)
    gram = jnp.where(line < SIDE, gram, square)
    return [jnp.where(lane % SIDE >= GROUP, jnp.broadcast_to(gram, shape), out) for out in outs]


def gram_of(totals):
    place = lane_of(totals.shape) // ROWS
    wanted = [GROUP // ROWS + i for i in range(KRYLOV)] + [(SIDE + GROUP) // ROWS]
    return [jnp.sum(jnp.where(place == at, totals, 0.0)) for at in wanted]


def unpacked(received, flat, tables):
    turned = received.T
    sides = []
    for dc in range(2):
        fields = turned[dc * SIDE : dc * SIDE + GROUP]
        sides.append(product(halves(fields), (tables[0, dc], tables[1, dc])))
    whole = jnp.concatenate([sides[0] + sides[1], reversed_lanes(sides[0] - sides[1])], 1)
    disp, rate, cut, edge = [whole[i * ROWS : (i + 1) * ROWS] for i in range(4)]
    return disp, rate - flat[:ROWS], flat[:ROWS] + edge, flat[ROWS:] + cut


def device_index():
    return lax.axis_index("tm") * 2 + lax.axis_index("rows")


def load_kernel(
    resid_hbm, basis_hbm, tables_hbm, symbol_hbm,
    fields_ref, give_ref, own_ref, tables_ref, symbol_ref, sems,
):
    pairs = [(resid_hbm.at[c, 0], fields_ref.at[pl.ds(c * ROWS, ROWS)]) for c in range(2)]
    for i in range(KRYLOV):
        pairs.append((basis_hbm.at[i, 1, 0], fields_ref.at[pl.ds((2 + i) * ROWS, ROWS)]))
    for i in range(KRYLOV):
        place = fields_ref.at[pl.ds((6 + i) * ROWS, ROWS)] if i < 2 else give_ref.at[pl.ds((i - 2) * ROWS, ROWS)]
        pairs.append((basis_hbm.at[i, 0, 0], place))
    pairs.append((symbol_hbm.at[pl.ds(device_index(), 1)], symbol_ref))
    pairs.append((tables_hbm, tables_ref))
    copies = [pltpu.make_async_copy(a, b, sems.at[i]) for i, (a, b) in enumerate(pairs)]
    for copy in copies:
        copy.start()
    for copy in copies[:-2]:
        copy.wait()
    own_ref[...] = own_products(fields_ref[...], give_ref[...])
    for copy in copies[-2:]:
        copy.wait()


def pack_kernel(fields_ref, lent_ref, tables_ref, send_ref):
    second = lax.axis_index("tm") == 1
    send_ref[...] = packed(fields_ref[...], lent_ref[...], second, tables_ref)


def solve_kernel(
    kappa, count, recv_ref, own_ref, symbol_ref, time_ref, enter_ref, leave_ref, send_ref
):
    steps = time_ref.shape[1]
    parts = [recv_ref[pl.ds(h, steps, stride=2), :] for h in range(2)]
    outs = solved(
        parts, own_ref[...], symbol_ref[...], time_ref, enter_ref, leave_ref, kappa, count
    )
    for h, out in enumerate(outs):
        send_ref[pl.ds(h, steps, stride=2), :] = out


def unpack_kernel(recv_ref, fields_ref, tables_ref, precond_ref, image_ref, gram_ref):
    received = recv_ref[...]
    flat = fields_ref[:MODES]
    fields = unpacked(received, flat, tables_ref)
    for slot, field in enumerate(fields):
        (precond_ref, image_ref)[slot // 2][slot % 2, 0] = field
    for i, value in enumerate(gram_of(jnp.sum(received, 0, keepdims=True))):
        gram_ref[i] = value


def solution(mesh):
    axes = ("tm", "rows")
    steps = mesh.shape["tm"]
    devices = steps * mesh.shape["rows"]
    params = pltpu.CompilerParams(vmem_limit_bytes=12 * 2**20)

    def on_device(resid, basis):
        cols = resid.shape[3]
        kappa = coupling(steps)
        count = 2.0 * steps * MODES * cols
        tables = both_halves(column_tables(cols))
        enter, leave = (both_halves(t) for t in row_tables())
        vmem = pl.BlockSpec(memory_space=pltpu.VMEM)
        hbm = pl.BlockSpec(memory_space=pltpu.HBM)
        symbol = jnp.asarray(symbol_table(cols))
        placed = [pltpu.with_memory_space_constraint(a, pltpu.HBM) for a in (resid, basis, tables, symbol)]
        message = jax.ShapeDtypeStruct((devices, LANES), jnp.float32)
        fields, give, own, tables, symbol = pl.pallas_call(
            load_kernel,
            in_specs=[hbm] * 4,
            out_shape=(
                jax.ShapeDtypeStruct((SIDE, cols), jnp.float32),
                jax.ShapeDtypeStruct((MODES, cols), jnp.float32),
                jax.ShapeDtypeStruct(((KRYLOV + 1) * ROWS, LANES), jnp.float32),
                jax.ShapeDtypeStruct(tables.shape, tables.dtype),
                jax.ShapeDtypeStruct((1, LANES), jnp.float32),
            ),
            scratch_shapes=[pltpu.SemaphoreType.DMA((2 + 2 * KRYLOV + 2,))],
            compiler_params=params,
            name="load",
        )(*placed)
        lent = lax.ppermute(give, "tm", [(0, 1)])
        send = pl.pallas_call(
            pack_kernel,
            out_shape=message,
            compiler_params=params,
            name="pack",
        )(fields, lent, tables)
        recv = lax.all_to_all(send, axes, 0, 0, tiled=True)
        back = pl.pallas_call(
            lambda *refs: solve_kernel(kappa, count, *refs),
            out_shape=message,
            compiler_params=params,
            name="solve",
        )(recv, own, symbol, both_halves(time_table(steps)), enter, leave)
        home = lax.all_to_all(back, axes, 0, 0, tiled=True)
        shard = jax.ShapeDtypeStruct(resid.shape, jnp.float32)
        precond, image, gram = pl.pallas_call(
            unpack_kernel,
            out_shape=(shard, shard, jax.ShapeDtypeStruct((KRYLOV + 1,), jnp.float32)),
            out_specs=(vmem, vmem, pl.BlockSpec(memory_space=pltpu.SMEM)),
            compiler_params=params,
            name="unpack",
        )(home, fields, tables)
        return precond, image, gram

    return jax.shard_map(
        on_device,
        mesh=mesh,
        in_specs=(P(None, "tm", "rows", None), P(None, None, "tm", "rows", None)),
        out_specs=(P(None, "tm", "rows", None), P(None, "tm", "rows", None), P()),
        check_vma=False,
    )
```

```python
import jax
import jax.numpy as jnp
import numpy as np
from jax import lax
from jax.experimental import pallas as pl
from jax.experimental.pallas import tpu as pltpu
from jax.sharding import PartitionSpec as P

ALPHA = 0.01
SWEEPS = 4
KRYLOV = 4
LANES = 128
ROWS = 8
SIDE = LANES // 2
MODES = 2 * ROWS
GROUP = 2 * MODES


def roll(value, amount, axis):
    size = value.shape[axis]
    return pltpu.roll(value, amount % size, axis)


def reversed_lanes(value):
    parts = [value[:, at : at + LANES] for at in range(0, value.shape[1], LANES)]
    index = LANES - 1 - lane_of(parts[0].shape)
    taken = [jnp.take_along_axis(p, index, axis=1, mode="promise_in_bounds") for p in parts]
    return jnp.concatenate(taken[::-1], 1)


def lane_of(shape):
    return lax.broadcasted_iota(jnp.int32, shape, len(shape) - 1)


def row_of(shape):
    return lax.broadcasted_iota(jnp.int32, shape, 0)


def sines(number, place, length):
    turn = np.outer(number, place + 1.0) / (length + 1)
    return np.sqrt(2.0 / (length + 1)) * np.sin(np.pi * turn)


def coupling(steps):
    return 16.0 / (steps * steps)


def time_table(steps):
    kappa = coupling(steps)
    index = np.arange(steps)
    gamma = ALPHA ** (index / steps)
    lam = 1.0 - ALPHA ** (1.0 / steps) * np.exp(-2j * np.pi * index / steps)
    den = lam * lam + 4.0 * kappa
    turn = np.exp(-2j * np.pi * np.outer(index, index) / steps)
    tables = []
    for m in range(SWEEPS):
        inner = np.conj(turn) @ ((1.0 / den ** (m + 1))[:, None] * turn) / steps
        tables.append(kappa**m * (inner.real / gamma[:, None]) * gamma[None, :])
    return np.concatenate(tables, 1)


def column_numbers(cols):
    return [2.0 * np.arange(cols // 2) + 1 + dc for dc in range(2)]


def column_tables(cols):
    return [sines(n, np.arange(cols // 2), cols) for n in column_numbers(cols)]


def symbol_table(cols):
    rows = 2.0 * np.cos(np.pi * (np.arange(MODES) + 1) / (MODES + 1))
    sums = []
    for number in column_numbers(cols):
        sums.append(2.0 * np.cos(np.pi * number / (cols + 1))[:, None] + rows[None, :])
    return np.tile(np.concatenate(sums, 1), (1, LANES // GROUP)).astype(np.float32)


def row_tables():
    wave = sines(np.arange(MODES) + 1, np.arange(MODES), MODES)
    enter = np.zeros((2, LANES, LANES))
    leave = np.zeros((LANES, 2, 2, LANES))
    for h in range(2):
        for row in range(ROWS):
            for dc in range(2):
                value = wave[:, h * ROWS + row]
                modes = dc * MODES + np.arange(MODES)
                for group in range(0, LANES, GROUP):
                    for c in range(2):
                        enter[h, dc * SIDE + c * ROWS + row, group + modes] = value
                for field, group in enumerate((0, 2, 1, 3)):
                    leave[group * GROUP + modes, 0, h, dc * SIDE + field * ROWS + row] = value
                for slot in (1, *range(KRYLOV, 2 * KRYLOV)):
                    leave[GROUP + modes, 1, h, dc * SIDE + slot * ROWS + row] = value
    return enter.reshape(2 * LANES, LANES), leave.reshape(LANES, 4 * LANES)


def halves(value):
    high = value.astype(jnp.bfloat16)
    return high, (value - high.astype(jnp.float32)).astype(jnp.bfloat16)


def both_halves(table):
    high = table.astype(jnp.bfloat16)
    return jnp.asarray(np.stack([high, (table - high.astype(np.float64)).astype(jnp.bfloat16)]))


def product(left, right, contract=((1,), (0,))):
    total = 0.0
    for i, j in ((1, 0), (0, 1), (0, 0)):
        total = total + lax.dot_general(
            left[i], right[j], (contract, ((), ())), preferred_element_type=jnp.float32
        )
    return total


def folded(fields, lent, second):
    half = fields.shape[1] // 2
    mixed = jnp.where(second, lent, fields[MODES : 2 * MODES])
    whole = jnp.concatenate([fields[:MODES], mixed, fields[2 * MODES :]], 0)
    left, right = whole[:, :half], reversed_lanes(whole[:, half:])
    return [halves(left + right), halves(left - right)]


def turned_to_modes(fold, table):
    return product(table, fold, ((1,), (1,)))


def own_products(fields, given):
    rows = [fields[at : at + ROWS] for at in range(0, fields.shape[0], ROWS)]
    given = [given[at : at + ROWS] for at in range(0, given.shape[0], ROWS)]
    disp, velo, firsts, seconds = rows[0], rows[1], rows[2:4] + given, rows[4:]
    terms = [f * disp + s * velo for f, s in zip(firsts, seconds)]
    terms.append(disp * disp + velo * velo)
    sums = [sum(t[:, at : at + LANES] for at in range(0, t.shape[1], LANES)) for t in terms]
    return jnp.concatenate(sums, 0)


def delayed(value):
    moved = roll(value, 1, 0)
    return jnp.where(row_of(value.shape) == 0, ALPHA * moved, moved)


def solved(parts, own, symbol, time, enter, leave, kappa, count):
    steps = parts[0].shape[0]
    shape = (steps, LANES)
    lane, row = lane_of(shape), row_of(shape)
    is_disp = lane % SIDE < ROWS
    mixed = [jnp.where(is_disp, x - delayed(x), x) for x in parts]
    source = product(halves(jnp.concatenate(mixed, 1)), enter)
    line = lane_of((1, LANES))
    cut = line // GROUP == 1
    power, weights = jnp.ones((1, LANES), jnp.float32), []
    for m in range(SWEEPS):
        last = -kappa * power * symbol if m == SWEEPS - 1 else 0.0
        weights.append(jnp.where(cut, last, power))
        power = power * symbol
    stack = jnp.concatenate([source * weight for weight in weights], 0)
    found = product(time, halves(stack))
    late = delayed(found)
    group = lane // GROUP
    found = jnp.where(group == 2, found - late, found)
    found = jnp.where(group == 3, jnp.where(row == 0, late, 0.0), found)
    spread = product(halves(found), leave)
    at = line % SIDE
    slot = at // ROWS
    outs, gram, square = [], 0.0, 0.0
    for h, x in enumerate(parts):
        out = spread[:, h * LANES : (h + 1) * LANES]
        gone = spread[:, (2 + h) * LANES : (3 + h) * LANES]
        ended = roll(out[steps - 1 :], ROWS, 1) - roll(x[steps - 1 :], 2 * ROWS, 1)
        rate = jnp.where(slot == 2, ALPHA * ended, 0.0)
        outs.append(jnp.where((row == 0) & (slot == 2), out + rate, out))
        disp = jnp.where(slot == 3, out[:1], 0.0)
        inner = jnp.sum(jnp.where(slot >= KRYLOV, x * gone, gone * (2.0 * x + gone)), 0, keepdims=True)
        wide = roll(rate, 2 * ROWS, 1) + roll(rate, 3 * ROWS, 1)
        wide = wide + roll(wide, 2 * ROWS, 1)
        tail = roll(disp, -ROWS, 1) + disp
        gram = gram + jnp.where(slot >= KRYLOV, inner + x[:1] * wide, 0.0)
        gram = gram + jnp.where((slot == 4) | (slot == 5), roll(x[:1] * tail, 2 * ROWS, 1), 0.0)
        gram = gram + jnp.where((slot == 6) | (slot == 7), roll(x[1:2] * tail, 4 * ROWS, 1), 0.0)
        rate, disp = roll(rate, -ROWS, 1), roll(disp, -3 * ROWS, 1)
        square = square + jnp.where(slot == 1, inner + rate * (2.0 * (x[:1] + gone[:1]) + rate), 0.0)
        square = square + jnp.where(slot == 0, disp * (2.0 * x[:1] + disp), 0.0)
    totals = [
        jnp.sum(jnp.sum(own[i * ROWS : (i + 1) * ROWS], 0, keepdims=True), 1, keepdims=True)
        for i in range(KRYLOV + 1)
    ]
    extra = jnp.where(line == SIDE + GROUP, totals[KRYLOV] * (1.0 / count), 0.0)
    for i in range(KRYLOV):
        extra = extra + jnp.where(line == GROUP + i * ROWS, totals[i], 0.0)
    square = square * (1.0 / count)
    square = roll(square, GROUP + SIDE, 1) + roll(square, GROUP, 1)
    gram = jnp.where(line < SIDE, gram + roll(gram, SIDE, 1), square) + extra
    return [jnp.where(lane % SIDE >= GROUP, jnp.broadcast_to(gram, shape), out) for out in outs]


def gram_of(totals):
    line = lane_of(totals.shape)
    masks = [line // ROWS == GROUP // ROWS + i for i in range(KRYLOV)]
    masks.append(line // MODES == (SIDE + GROUP) // MODES)
    return [jnp.sum(jnp.where(mask, totals, 0.0)) for mask in masks]


def unpacked(received, flat, tables):
    turned = received.T
    sides = []
    for dc in range(2):
        fields = turned[dc * SIDE : dc * SIDE + GROUP]
        sides.append(product(halves(fields), tables[dc]))
    whole = jnp.concatenate([sides[0] + sides[1], reversed_lanes(sides[0] - sides[1])], 1)
    disp, rate, cut, edge = [whole[i * ROWS : (i + 1) * ROWS] for i in range(4)]
    return disp, rate - flat[:ROWS], flat[:ROWS] + edge, flat[ROWS:] + cut


def device_index():
    return lax.axis_index("tm") * 2 + lax.axis_index("rows")


def pack_kernel(
    resid_hbm, basis_hbm, tables_hbm, symbol_hbm, lent_ref,
    send_ref, own_ref, fields_ref, tables_ref, symbol_ref, given_ref, sems,
):
    slabs = [fields_ref.at[pl.ds(at, ROWS)] for at in range(0, SIDE, ROWS)]
    pairs = [(resid_hbm.at[c, 0], slabs[c]) for c in range(2)]
    for i in range(KRYLOV):
        place = slabs[2 + i] if i < 2 else given_ref.at[pl.ds((i - 2) * ROWS, ROWS)]
        pairs.append((basis_hbm.at[i, 0, 0], place))
        pairs.append((basis_hbm.at[i, 1, 0], slabs[4 + i]))
    for dc in range(2):
        pairs.append((tables_hbm.at[dc], tables_ref.at[dc]))
    pairs.append((symbol_hbm.at[pl.ds(device_index(), 1)], symbol_ref))
    copies = [pltpu.make_async_copy(a, b, sems.at[i]) for i, (a, b) in enumerate(pairs)]
    for copy in copies:
        copy.start()
    second = lax.axis_index("tm") == 1
    for copy in copies[:-3]:
        copy.wait()
    fields = fields_ref[...]
    folds = folded(fields, lent_ref[2:, 0, 0].reshape(MODES, fields.shape[1]), second)
    own_ref[...] = own_products(fields, given_ref[...])
    sides = []
    for dc in range(2):
        copies[dc - 3].wait()
        sides.append(turned_to_modes(folds[dc], tables_ref[dc]))
    send_ref[...] = jnp.concatenate(sides, 1)
    copies[-1].wait()


def solve_kernel(
    kappa, count, recv_ref, own_ref, symbol_ref, time_ref, enter_ref, leave_ref, send_ref
):
    steps = time_ref.shape[1]
    parts = [recv_ref[pl.ds(h, steps, stride=2), :] for h in range(2)]
    outs = solved(
        parts, own_ref[...], symbol_ref[...], time_ref, enter_ref, leave_ref, kappa, count
    )
    for h, out in enumerate(outs):
        send_ref[pl.ds(h, steps, stride=2), :] = out


def unpack_kernel(
    recv_ref, fields_ref, tables_ref, precond_hbm, image_hbm, gram_hbm, whole_ref, gram_ref, sems
):
    received = recv_ref[...]
    fields = unpacked(received, fields_ref[:MODES], tables_ref)
    copies = []
    for slot, field in enumerate(fields):
        whole_ref[slot] = field
        target = (precond_hbm, image_hbm)[slot // 2].at[slot % 2, 0]
        copies.append(pltpu.make_async_copy(whole_ref.at[slot], target, sems.at[slot]))
        copies[-1].start()
    for i, value in enumerate(gram_of(jnp.sum(received, 0, keepdims=True))):
        gram_ref[i] = value
    copies.append(pltpu.make_async_copy(gram_ref, gram_hbm, sems.at[len(fields)]))
    copies[-1].start()
    for copy in copies:
        copy.wait()


def solution(mesh):
    axes = ("tm", "rows")
    steps = mesh.shape["tm"]
    devices = steps * mesh.shape["rows"]
    params = pltpu.CompilerParams(vmem_limit_bytes=12 * 2**20)

    def on_device(resid, basis):
        cols = resid.shape[3]
        kappa = coupling(steps)
        count = 2.0 * steps * MODES * cols
        tables = jnp.stack([both_halves(t) for t in column_tables(cols)])
        enter, leave = (both_halves(t) for t in row_tables())
        vmem = pl.BlockSpec(memory_space=pltpu.VMEM)
        hbm = pl.BlockSpec(memory_space=pltpu.HBM)
        symbol = jnp.asarray(symbol_table(cols))
        placed = [pltpu.with_memory_space_constraint(a, pltpu.HBM) for a in (resid, basis, tables, symbol)]
        message = jax.ShapeDtypeStruct((devices, LANES), jnp.float32)
        lent = lax.ppermute(basis, "tm", [(0, 1)])
        send, own, fields, tables, symbol = pl.pallas_call(
            pack_kernel,
            in_specs=[hbm] * 4 + [vmem],
            out_shape=(
                message,
                jax.ShapeDtypeStruct(((KRYLOV + 1) * ROWS, LANES), jnp.float32),
                jax.ShapeDtypeStruct((SIDE, cols), jnp.float32),
                jax.ShapeDtypeStruct(tables.shape, tables.dtype),
                jax.ShapeDtypeStruct((1, LANES), jnp.float32),
            ),
            scratch_shapes=[
                pltpu.VMEM((MODES, cols), jnp.float32),
                pltpu.SemaphoreType.DMA((2 + 2 * KRYLOV + 3,)),
            ],
            compiler_params=params,
            name="pack",
        )(*placed, lent)
        recv = lax.all_to_all(send, axes, 0, 0, tiled=True)
        back = pl.pallas_call(
            lambda *refs: solve_kernel(kappa, count, *refs),
            out_shape=message,
            compiler_params=params,
            name="solve",
        )(recv, own, symbol, both_halves(time_table(steps)), enter, leave)
        home = lax.all_to_all(back, axes, 0, 0, tiled=True)
        shard = jax.ShapeDtypeStruct(resid.shape, jnp.float32)
        precond, image, gram = pl.pallas_call(
            unpack_kernel,
            out_shape=(shard, shard, jax.ShapeDtypeStruct((KRYLOV + 1,), jnp.float32)),
            in_specs=[vmem] * 3,
            out_specs=[hbm] * 3,
            scratch_shapes=[
                pltpu.VMEM((4, ROWS, cols), jnp.float32),
                pltpu.SMEM((KRYLOV + 1,), jnp.float32),
                pltpu.SemaphoreType.DMA((5,)),
            ],
            compiler_params=params,
            name="unpack",
        )(home, fields, tables)
        return precond, image, gram

    return jax.shard_map(
        on_device,
        mesh=mesh,
        in_specs=(P(None, "tm", "rows", None), P(None, None, "tm", "rows", None)),
        out_specs=(P(None, "tm", "rows", None), P(None, "tm", "rows", None), P()),
        check_vma=False,
    )
```

```python
import jax
import jax.numpy as jnp
import numpy as np
from jax import lax
from jax.experimental import pallas as pl
from jax.experimental.pallas import tpu as pltpu
from jax.sharding import PartitionSpec as P

ALPHA = 0.01
SWEEPS = 4
KRYLOV = 4
LANES = 128
ROWS = 8
SIDE = LANES // 2
MODES = 2 * ROWS
GROUP = 2 * MODES


def roll(value, amount, axis):
    size = value.shape[axis]
    return pltpu.roll(value, amount % size, axis)


def reversed_lanes(value):
    parts = [value[:, at : at + LANES] for at in range(0, value.shape[1], LANES)]
    index = LANES - 1 - lane_of(parts[0].shape)
    taken = [jnp.take_along_axis(p, index, axis=1, mode="promise_in_bounds") for p in parts]
    return jnp.concatenate(taken[::-1], 1)


def lane_of(shape):
    return lax.broadcasted_iota(jnp.int32, shape, len(shape) - 1)


def row_of(shape):
    return lax.broadcasted_iota(jnp.int32, shape, 0)


def sines(number, place, length):
    turn = np.outer(number, place + 1.0) / (length + 1)
    return np.sqrt(2.0 / (length + 1)) * np.sin(np.pi * turn)


def coupling(steps):
    return 16.0 / (steps * steps)


def time_table(steps):
    kappa = coupling(steps)
    index = np.arange(steps)
    gamma = ALPHA ** (index / steps)
    lam = 1.0 - ALPHA ** (1.0 / steps) * np.exp(-2j * np.pi * index / steps)
    den = lam * lam + 4.0 * kappa
    turn = np.exp(-2j * np.pi * np.outer(index, index) / steps)
    tables = []
    for m in range(SWEEPS):
        inner = np.conj(turn) @ ((1.0 / den ** (m + 1))[:, None] * turn) / steps
        tables.append(kappa**m * (inner.real / gamma[:, None]) * gamma[None, :])
    return np.concatenate(tables, 1)


def column_numbers(cols):
    return [2.0 * np.arange(cols // 2) + 1 + dc for dc in range(2)]


def column_tables(cols):
    return [sines(n, np.arange(cols // 2), cols) for n in column_numbers(cols)]


def symbol_table(cols):
    rows = 2.0 * np.cos(np.pi * (np.arange(MODES) + 1) / (MODES + 1))
    sums = []
    for number in column_numbers(cols):
        sums.append(2.0 * np.cos(np.pi * number / (cols + 1))[:, None] + rows[None, :])
    return np.tile(np.concatenate(sums, 1), (1, LANES // GROUP)).astype(np.float32)


def row_tables():
    wave = sines(np.arange(MODES) + 1, np.arange(MODES), MODES)
    enter = np.zeros((2, LANES, LANES))
    leave = np.zeros((LANES, 2, 2, LANES))
    for h in range(2):
        for row in range(ROWS):
            for dc in range(2):
                value = wave[:, h * ROWS + row]
                modes = dc * MODES + np.arange(MODES)
                for group in range(0, LANES, GROUP):
                    for c in range(2):
                        enter[h, dc * SIDE + c * ROWS + row, group + modes] = value
                for field, group in enumerate((0, 2, 1, 3)):
                    leave[group * GROUP + modes, 0, h, dc * SIDE + field * ROWS + row] = value
                for slot in (1, *range(KRYLOV, 2 * KRYLOV)):
                    leave[GROUP + modes, 1, h, dc * SIDE + slot * ROWS + row] = value
    enter = enter.reshape(4, SIDE, LANES).transpose(1, 0, 2).reshape(SIDE, 4 * LANES)
    return leave.reshape(LANES, 4 * LANES), enter


def halves(value):
    high = value.astype(jnp.bfloat16)
    return high, (value - high.astype(jnp.float32)).astype(jnp.bfloat16)


def both_halves(table):
    high = table.astype(jnp.bfloat16)
    return jnp.asarray(np.stack([high, (table - high.astype(np.float64)).astype(jnp.bfloat16)]))


def product(left, right, contract=((1,), (0,))):
    total = 0.0
    for i, j in ((1, 0), (0, 1), (0, 0)):
        total = total + lax.dot_general(
            left[i], right[j], (contract, ((), ())), preferred_element_type=jnp.float32
        )
    return total


def folded(flat, basis, lent, second):
    half = flat.shape[1] // 2
    mixed = [jnp.where(second, lent[i], basis[i, 0]) for i in range(2)]
    whole = jnp.concatenate([flat] + mixed + [basis[i, 1] for i in range(KRYLOV)], 0)
    left, right = whole[:, :half], reversed_lanes(whole[:, half:])
    return [halves(left + right), halves(left - right)]


def turned_to_modes(fold, table):
    return product(table, fold, ((1,), (1,)))


def own_products(flat, basis):
    disp, velo = flat[:ROWS], flat[ROWS:]
    terms = [basis[i, 0] * disp + basis[i, 1] * velo for i in range(KRYLOV)]
    terms.append(disp * disp + velo * velo)
    sums = [sum(t[:, at : at + LANES] for at in range(0, t.shape[1], LANES)) for t in terms]
    return jnp.concatenate(sums, 0)


def delayed(value):
    moved = roll(value, 1, 0)
    return jnp.where(row_of(value.shape) == 0, ALPHA * moved, moved)


def solved(parts, own, symbol, time, enter, leave, kappa, count):
    steps = parts[0].shape[0]
    shape = (steps, LANES)
    lane, row = lane_of(shape), row_of(shape)
    is_disp = lane % SIDE < ROWS
    mixed = [jnp.where(is_disp, x - delayed(x), x) for x in parts]
    source = product(halves(jnp.concatenate(mixed, 1)), enter)
    line = lane_of((1, LANES))
    cut = line // GROUP == 1
    power, weights = jnp.ones((1, LANES), jnp.float32), []
    for m in range(SWEEPS):
        last = -kappa * power * symbol if m == SWEEPS - 1 else 0.0
        weights.append(jnp.where(cut, last, power))
        power = power * symbol
    stack = jnp.concatenate([source * weight for weight in weights], 0)
    found = product(time, halves(stack))
    late = delayed(found)
    group = lane // GROUP
    found = jnp.where(group == 2, found - late, found)
    found = jnp.where(group == 3, jnp.where(row == 0, late, 0.0), found)
    spread = product(halves(found), leave)
    at = line % SIDE
    slot = at // ROWS
    outs, gram, square = [], 0.0, 0.0
    for h, x in enumerate(parts):
        out = spread[:, h * LANES : (h + 1) * LANES]
        gone = spread[:, (2 + h) * LANES : (3 + h) * LANES]
        ended = roll(out[steps - 1 :], ROWS, 1) - roll(x[steps - 1 :], 2 * ROWS, 1)
        rate = jnp.where(slot == 2, ALPHA * ended, 0.0)
        outs.append(jnp.where((row == 0) & (slot == 2), out + rate, out))
        disp = jnp.where(slot == 3, out[:1], 0.0)
        inner = jnp.sum(jnp.where(slot >= KRYLOV, x * gone, gone * (2.0 * x + gone)), 0, keepdims=True)
        wide = roll(rate, 2 * ROWS, 1) + roll(rate, 3 * ROWS, 1)
        wide = wide + roll(wide, 2 * ROWS, 1)
        tail = roll(disp, -ROWS, 1) + disp
        gram = gram + jnp.where(slot >= KRYLOV, inner + x[:1] * wide, 0.0)
        gram = gram + jnp.where((slot == 4) | (slot == 5), roll(x[:1] * tail, 2 * ROWS, 1), 0.0)
        gram = gram + jnp.where((slot == 6) | (slot == 7), roll(x[1:2] * tail, 4 * ROWS, 1), 0.0)
        rate, disp = roll(rate, -ROWS, 1), roll(disp, -3 * ROWS, 1)
        square = square + jnp.where(slot == 1, inner + rate * (2.0 * (x[:1] + gone[:1]) + rate), 0.0)
        square = square + jnp.where(slot == 0, disp * (2.0 * x[:1] + disp), 0.0)
    totals = [
        jnp.sum(jnp.sum(own[i * ROWS : (i + 1) * ROWS], 0, keepdims=True), 1, keepdims=True)
        for i in range(KRYLOV + 1)
    ]
    extra = jnp.where(line == SIDE + GROUP, totals[KRYLOV] * (1.0 / count), 0.0)
    for i in range(KRYLOV):
        extra = extra + jnp.where(line == GROUP + i * ROWS, totals[i], 0.0)
    square = square * (1.0 / count)
    square = roll(square, GROUP + SIDE, 1) + roll(square, GROUP, 1)
    gram = jnp.where(line < SIDE, gram + roll(gram, SIDE, 1), square) + extra
    return [jnp.where(lane % SIDE >= GROUP, jnp.broadcast_to(gram, shape), out) for out in outs]


def gram_of(totals):
    line = lane_of(totals.shape)
    masks = [line // ROWS == GROUP // ROWS + i for i in range(KRYLOV)]
    masks.append(line // MODES == (SIDE + GROUP) // MODES)
    return [jnp.sum(jnp.where(mask, totals, 0.0)) for mask in masks]


def unpacked(received, flat, tables):
    turned = received.T
    sides = []
    for dc in range(2):
        fields = turned[dc * SIDE : dc * SIDE + GROUP]
        sides.append(product(halves(fields), tables[dc]))
    whole = jnp.concatenate([sides[0] + sides[1], reversed_lanes(sides[0] - sides[1])], 1)
    disp, rate, cut, edge = [whole[i * ROWS : (i + 1) * ROWS] for i in range(4)]
    return disp, rate - flat[:ROWS], flat[:ROWS] + edge, flat[ROWS:] + cut


def device_index():
    return lax.axis_index("tm") * 2 + lax.axis_index("rows")


def pack_kernel(
    resid_hbm, basis_hbm, tables_hbm, symbol_hbm, lent_ref,
    send_ref, own_ref, resid_ref, tables_ref, symbol_ref, basis_ref, sems,
):
    pairs = (
        (resid_hbm, resid_ref),
        (basis_hbm, basis_ref),
        (tables_hbm, tables_ref),
        (symbol_hbm.at[pl.ds(device_index(), 1)], symbol_ref),
    )
    copies = [pltpu.make_async_copy(a, b, sems.at[i]) for i, (a, b) in enumerate(pairs)]
    for copy in copies:
        copy.start()
    second = lax.axis_index("tm") == 1
    copies[0].wait()
    copies[1].wait()
    flat = resid_ref[...].reshape(MODES, resid_ref.shape[-1])
    basis = basis_ref[:, :, 0]
    folds = folded(flat, basis, lent_ref[2:, 0, 0], second)
    own_ref[...] = own_products(flat, basis)
    copies[2].wait()
    sides = [turned_to_modes(folds[dc], tables_ref[dc]) for dc in range(2)]
    send_ref[...] = jnp.concatenate(sides, 1)
    copies[3].wait()


def solve_kernel(
    kappa, count, steps, recv_ref, own_ref, symbol_ref, tables_ref, send_ref
):
    time, leave = tables_ref[:, :steps], tables_ref[:, steps : steps + LANES]
    stored = tables_ref[:, steps + LANES :]
    enter = jnp.concatenate([stored[:, :, at : at + LANES] for at in range(0, 4 * LANES, LANES)], 1)
    parts = [recv_ref[pl.ds(h, steps, stride=2), :] for h in range(2)]
    outs = solved(
        parts, own_ref[...], symbol_ref[...], time, enter, leave, kappa, count
    )
    for h, out in enumerate(outs):
        send_ref[pl.ds(h, steps, stride=2), :] = out


def unpack_kernel(recv_ref, resid_ref, tables_ref, precond_ref, image_ref, gram_ref):
    received = recv_ref[...]
    flat = resid_ref[...].reshape(MODES, resid_ref.shape[-1])
    for slot, field in enumerate(unpacked(received, flat, tables_ref)):
        (precond_ref, image_ref)[slot // 2][slot % 2, 0] = field
    for i, value in enumerate(gram_of(jnp.sum(received, 0, keepdims=True))):
        gram_ref[i] = value


def solution(mesh):
    axes = ("tm", "rows")
    steps = mesh.shape["tm"]
    devices = steps * mesh.shape["rows"]
    params = pltpu.CompilerParams(vmem_limit_bytes=12 * 2**20)

    def on_device(resid, basis):
        cols = resid.shape[3]
        kappa = coupling(steps)
        count = 2.0 * steps * MODES * cols
        tables = jnp.stack([both_halves(t) for t in column_tables(cols)])
        solve_tables = both_halves(np.concatenate([time_table(steps), *row_tables()], 0))
        vmem = pl.BlockSpec(memory_space=pltpu.VMEM)
        hbm = pl.BlockSpec(memory_space=pltpu.HBM)
        symbol = jnp.asarray(symbol_table(cols))
        placed = [pltpu.with_memory_space_constraint(a, pltpu.HBM) for a in (resid, basis, tables, symbol)]
        message = jax.ShapeDtypeStruct((devices, LANES), jnp.float32)
        lent = lax.ppermute(basis, "tm", [(0, 1)])
        send, own, kept, tables, symbol = pl.pallas_call(
            pack_kernel,
            in_specs=[hbm] * 4 + [vmem],
            out_shape=(
                message,
                jax.ShapeDtypeStruct(((KRYLOV + 1) * ROWS, LANES), jnp.float32),
                jax.ShapeDtypeStruct(resid.shape, jnp.float32),
                jax.ShapeDtypeStruct(tables.shape, tables.dtype),
                jax.ShapeDtypeStruct((1, LANES), jnp.float32),
            ),
            scratch_shapes=[
                pltpu.VMEM(basis.shape, jnp.float32),
                pltpu.SemaphoreType.DMA((4,)),
            ],
            compiler_params=params,
            name="pack",
        )(*placed, lent)
        recv = lax.all_to_all(send, axes, 0, 0, tiled=True)
        back = pl.pallas_call(
            lambda *refs: solve_kernel(kappa, count, steps, *refs),
            out_shape=message,
            compiler_params=params,
            name="solve",
        )(recv, own, symbol, solve_tables)
        home = lax.all_to_all(back, axes, 0, 0, tiled=True)
        shard = jax.ShapeDtypeStruct(resid.shape, jnp.float32)
        precond, image, gram = pl.pallas_call(
            unpack_kernel,
            out_shape=(shard, shard, jax.ShapeDtypeStruct((KRYLOV + 1,), jnp.float32)),
            out_specs=(vmem, vmem, pl.BlockSpec(memory_space=pltpu.SMEM)),
            compiler_params=params,
            name="unpack",
        )(home, kept, tables)
        return precond, image, gram

    return jax.shard_map(
        on_device,
        mesh=mesh,
        in_specs=(P(None, "tm", "rows", None), P(None, None, "tm", "rows", None)),
        out_specs=(P(None, "tm", "rows", None), P(None, "tm", "rows", None), P()),
        check_vma=False,
    )
```

```python
import jax
import jax.numpy as jnp
import numpy as np
from jax import lax
from jax.experimental import pallas as pl
from jax.experimental.pallas import tpu as pltpu
from jax.sharding import PartitionSpec as P

ALPHA = 0.01
SWEEPS = 4
KRYLOV = 4
LANES = 128
ROWS = 8
SIDE = LANES // 2
MODES = 2 * ROWS
GROUP = 2 * MODES


def roll(value, amount, axis):
    size = value.shape[axis]
    return pltpu.roll(value, amount % size, axis)


def reversed_lanes(value):
    parts = [value[:, at : at + LANES] for at in range(0, value.shape[1], LANES)]
    index = LANES - 1 - lane_of(parts[0].shape)
    taken = [jnp.take_along_axis(p, index, axis=1, mode="promise_in_bounds") for p in parts]
    return jnp.concatenate(taken[::-1], 1)


def lane_of(shape):
    return lax.broadcasted_iota(jnp.int32, shape, len(shape) - 1)


def row_of(shape):
    return lax.broadcasted_iota(jnp.int32, shape, 0)


def sines(number, place, length):
    turn = np.outer(number, place + 1.0) / (length + 1)
    return np.sqrt(2.0 / (length + 1)) * np.sin(np.pi * turn)


def coupling(steps):
    return 16.0 / (steps * steps)


def time_table(steps):
    kappa = coupling(steps)
    index = np.arange(steps)
    gamma = ALPHA ** (index / steps)
    lam = 1.0 - ALPHA ** (1.0 / steps) * np.exp(-2j * np.pi * index / steps)
    den = lam * lam + 4.0 * kappa
    turn = np.exp(-2j * np.pi * np.outer(index, index) / steps)
    tables = []
    for m in range(SWEEPS):
        inner = np.conj(turn) @ ((1.0 / den ** (m + 1))[:, None] * turn) / steps
        tables.append(kappa**m * (inner.real / gamma[:, None]) * gamma[None, :])
    return np.concatenate(tables, 1)


def column_numbers(cols):
    return [2.0 * np.arange(cols // 2) + 1 + dc for dc in range(2)]


def column_tables(cols):
    return [sines(n, np.arange(cols // 2), cols) for n in column_numbers(cols)]


def symbol_table(cols):
    rows = 2.0 * np.cos(np.pi * (np.arange(MODES) + 1) / (MODES + 1))
    sums = []
    for number in column_numbers(cols):
        sums.append(2.0 * np.cos(np.pi * number / (cols + 1))[:, None] + rows[None, :])
    return np.tile(np.concatenate(sums, 1), (1, LANES // GROUP)).astype(np.float32)


def row_tables():
    wave = sines(np.arange(MODES) + 1, np.arange(MODES), MODES)
    enter = np.zeros((2, LANES, LANES))
    leave = np.zeros((LANES, 2, 2, LANES))
    for h in range(2):
        for row in range(ROWS):
            for dc in range(2):
                value = wave[:, h * ROWS + row]
                modes = dc * MODES + np.arange(MODES)
                for group in range(0, LANES, GROUP):
                    for c in range(2):
                        enter[h, dc * SIDE + c * ROWS + row, group + modes] = value
                for field, group in enumerate((0, 2, 1, 3)):
                    leave[group * GROUP + modes, 0, h, dc * SIDE + field * ROWS + row] = value
                for slot in (1, *range(KRYLOV, 2 * KRYLOV)):
                    leave[GROUP + modes, 1, h, dc * SIDE + slot * ROWS + row] = value
    enter = enter.reshape(4, SIDE, LANES).transpose(1, 0, 2).reshape(SIDE, 4 * LANES)
    return leave.reshape(LANES, 4 * LANES), enter


def halves(value):
    high = value.astype(jnp.bfloat16)
    return high, (value - high.astype(jnp.float32)).astype(jnp.bfloat16)


def both_halves(table):
    high = table.astype(jnp.bfloat16)
    return jnp.asarray(np.stack([high, (table - high.astype(np.float64)).astype(jnp.bfloat16)]))


def dot(left, right, contract):
    return lax.dot_general(left, right, (contract, ((), ())), preferred_element_type=jnp.float32)


def product(left, right, contract=((1,), (0,))):
    rows = left[0].shape[0]
    both = dot(jnp.concatenate([left[0], left[1]], 0), right[0], contract)
    return both[:rows] + (both[rows:] + dot(left[0], right[1], contract))


def folded(flat, basis, lent, second):
    half = flat.shape[1] // 2
    mixed = [jnp.where(second, lent[i], basis[i, 0]) for i in range(2)]
    whole = jnp.concatenate([flat] + mixed + [basis[i, 1] for i in range(KRYLOV)], 0)
    left, right = whole[:, :half], reversed_lanes(whole[:, half:])
    return [halves(left + right), halves(left - right)]


def turned_to_modes(fold, table):
    return product(table, fold, ((1,), (1,)))


def own_products(flat, basis):
    disp, velo = flat[:ROWS], flat[ROWS:]
    terms = [basis[i, 0] * disp + basis[i, 1] * velo for i in range(KRYLOV)]
    terms.append(disp * disp + velo * velo)
    sums = [sum(t[:, at : at + LANES] for at in range(0, t.shape[1], LANES)) for t in terms]
    return jnp.concatenate(sums, 0)


def delayed(value):
    moved = roll(value, 1, 0)
    return jnp.where(row_of(value.shape) == 0, ALPHA * moved, moved)


def solved(parts, own, symbol, time, enter, leave, kappa, count):
    steps = parts[0].shape[0]
    shape = (steps, LANES)
    lane, row = lane_of(shape), row_of(shape)
    is_disp = lane % SIDE < ROWS
    mixed = [jnp.where(is_disp, x - delayed(x), x) for x in parts]
    source = product(halves(jnp.concatenate(mixed, 1)), enter)
    line = lane_of((1, LANES))
    cut = line // GROUP == 1
    power, weights = jnp.ones((1, LANES), jnp.float32), []
    for m in range(SWEEPS):
        last = -kappa * power * symbol if m == SWEEPS - 1 else 0.0
        weights.append(jnp.where(cut, last, power))
        power = power * symbol
    stack = jnp.concatenate([source * weight for weight in weights], 0)
    found = product(time, halves(stack))
    late = delayed(found)
    group = lane // GROUP
    found = jnp.where(group == 2, found - late, found)
    found = jnp.where(group == 3, jnp.where(row == 0, late, 0.0), found)
    spread = product(halves(found), leave)
    at = line % SIDE
    slot = at // ROWS
    outs, gram, square = [], 0.0, 0.0
    for h, x in enumerate(parts):
        out = spread[:, h * LANES : (h + 1) * LANES]
        gone = spread[:, (2 + h) * LANES : (3 + h) * LANES]
        ended = roll(out[steps - 1 :], ROWS, 1) - roll(x[steps - 1 :], 2 * ROWS, 1)
        rate = jnp.where(slot == 2, ALPHA * ended, 0.0)
        outs.append(jnp.where((row == 0) & (slot == 2), out + rate, out))
        disp = jnp.where(slot == 3, out[:1], 0.0)
        inner = jnp.sum(jnp.where(slot >= KRYLOV, x * gone, gone * (2.0 * x + gone)), 0, keepdims=True)
        wide = roll(rate, 2 * ROWS, 1) + roll(rate, 3 * ROWS, 1)
        wide = wide + roll(wide, 2 * ROWS, 1)
        tail = roll(disp, -ROWS, 1) + disp
        gram = gram + jnp.where(slot >= KRYLOV, inner + x[:1] * wide, 0.0)
        gram = gram + jnp.where((slot == 4) | (slot == 5), roll(x[:1] * tail, 2 * ROWS, 1), 0.0)
        gram = gram + jnp.where((slot == 6) | (slot == 7), roll(x[1:2] * tail, 4 * ROWS, 1), 0.0)
        rate, disp = roll(rate, -ROWS, 1), roll(disp, -3 * ROWS, 1)
        square = square + jnp.where(slot == 1, inner + rate * (2.0 * (x[:1] + gone[:1]) + rate), 0.0)
        square = square + jnp.where(slot == 0, disp * (2.0 * x[:1] + disp), 0.0)
    totals = [
        jnp.sum(jnp.sum(own[i * ROWS : (i + 1) * ROWS], 0, keepdims=True), 1, keepdims=True)
        for i in range(KRYLOV + 1)
    ]
    extra = jnp.where(line == SIDE + GROUP, totals[KRYLOV] * (1.0 / count), 0.0)
    for i in range(KRYLOV):
        extra = extra + jnp.where(line == GROUP + i * ROWS, totals[i], 0.0)
    square = square * (1.0 / count)
    square = roll(square, GROUP + SIDE, 1) + roll(square, GROUP, 1)
    gram = jnp.where(line < SIDE, gram + roll(gram, SIDE, 1), square) + extra
    return [jnp.where(lane % SIDE >= GROUP, jnp.broadcast_to(gram, shape), out) for out in outs]


def gram_of(totals):
    line = lane_of(totals.shape)
    masks = [line // ROWS == GROUP // ROWS + i for i in range(KRYLOV)]
    masks.append(line // MODES == (SIDE + GROUP) // MODES)
    return [jnp.sum(jnp.where(mask, totals, 0.0)) for mask in masks]


def unpacked(received, flat, tables):
    turned = received.T
    sides = []
    for dc in range(2):
        fields = turned[dc * SIDE : dc * SIDE + GROUP]
        sides.append(product(halves(fields), tables[dc]))
    whole = jnp.concatenate([sides[0] + sides[1], reversed_lanes(sides[0] - sides[1])], 1)
    disp, rate, cut, edge = [whole[i * ROWS : (i + 1) * ROWS] for i in range(4)]
    return disp, rate - flat[:ROWS], flat[:ROWS] + edge, flat[ROWS:] + cut


def device_index():
    return lax.axis_index("tm") * 2 + lax.axis_index("rows")


def pack_kernel(
    resid_hbm, basis_hbm, tables_hbm, symbol_hbm, lent_ref,
    send_ref, own_ref, resid_ref, tables_ref, symbol_ref, basis_ref, sems,
):
    pairs = (
        (resid_hbm, resid_ref),
        (basis_hbm, basis_ref),
        (tables_hbm, tables_ref),
        (symbol_hbm.at[pl.ds(device_index(), 1)], symbol_ref),
    )
    copies = [pltpu.make_async_copy(a, b, sems.at[i]) for i, (a, b) in enumerate(pairs)]
    for copy in copies:
        copy.start()
    second = lax.axis_index("tm") == 1
    copies[0].wait()
    copies[1].wait()
    flat = resid_ref[...].reshape(MODES, resid_ref.shape[-1])
    basis = basis_ref[:, :, 0]
    folds = folded(flat, basis, lent_ref[2:, 0, 0], second)
    own_ref[...] = own_products(flat, basis)
    copies[2].wait()
    sides = [turned_to_modes(folds[dc], tables_ref[dc]) for dc in range(2)]
    send_ref[...] = jnp.concatenate(sides, 1)
    copies[3].wait()


def solve_kernel(
    kappa, count, steps, recv_ref, own_ref, symbol_ref, tables_ref, send_ref
):
    time, leave = tables_ref[:, :steps], tables_ref[:, steps : steps + LANES]
    stored = tables_ref[:, steps + LANES :]
    enter = jnp.concatenate([stored[:, :, at : at + LANES] for at in range(0, 4 * LANES, LANES)], 1)
    parts = [recv_ref[pl.ds(h, steps, stride=2), :] for h in range(2)]
    outs = solved(
        parts, own_ref[...], symbol_ref[...], time, enter, leave, kappa, count
    )
    for h, out in enumerate(outs):
        send_ref[pl.ds(h, steps, stride=2), :] = out


def unpack_kernel(recv_ref, resid_ref, tables_ref, precond_ref, image_ref, gram_ref):
    received = recv_ref[...]
    flat = resid_ref[...].reshape(MODES, resid_ref.shape[-1])
    for slot, field in enumerate(unpacked(received, flat, tables_ref)):
        (precond_ref, image_ref)[slot // 2][slot % 2, 0] = field
    for i, value in enumerate(gram_of(jnp.sum(received, 0, keepdims=True))):
        gram_ref[i] = value


def solution(mesh):
    axes = ("tm", "rows")
    steps = mesh.shape["tm"]
    devices = steps * mesh.shape["rows"]
    params = pltpu.CompilerParams(vmem_limit_bytes=12 * 2**20)

    def on_device(resid, basis):
        cols = resid.shape[3]
        kappa = coupling(steps)
        count = 2.0 * steps * MODES * cols
        tables = jnp.stack([both_halves(t) for t in column_tables(cols)])
        solve_tables = both_halves(np.concatenate([time_table(steps), *row_tables()], 0))
        vmem = pl.BlockSpec(memory_space=pltpu.VMEM)
        hbm = pl.BlockSpec(memory_space=pltpu.HBM)
        symbol = jnp.asarray(symbol_table(cols))
        placed = [pltpu.with_memory_space_constraint(a, pltpu.HBM) for a in (resid, basis, tables, symbol)]
        message = jax.ShapeDtypeStruct((devices, LANES), jnp.float32)
        lent = lax.ppermute(basis, "tm", [(0, 1)])
        send, own, kept, tables, symbol = pl.pallas_call(
            pack_kernel,
            in_specs=[hbm] * 4 + [vmem],
            out_shape=(
                message,
                jax.ShapeDtypeStruct(((KRYLOV + 1) * ROWS, LANES), jnp.float32),
                jax.ShapeDtypeStruct(resid.shape, jnp.float32),
                jax.ShapeDtypeStruct(tables.shape, tables.dtype),
                jax.ShapeDtypeStruct((1, LANES), jnp.float32),
            ),
            scratch_shapes=[
                pltpu.VMEM(basis.shape, jnp.float32),
                pltpu.SemaphoreType.DMA((4,)),
            ],
            compiler_params=params,
            name="pack",
        )(*placed, lent)
        recv = lax.all_to_all(send, axes, 0, 0, tiled=True)
        back = pl.pallas_call(
            lambda *refs: solve_kernel(kappa, count, steps, *refs),
            out_shape=message,
            compiler_params=params,
            name="solve",
        )(recv, own, symbol, solve_tables)
        home = lax.all_to_all(back, axes, 0, 0, tiled=True)
        shard = jax.ShapeDtypeStruct(resid.shape, jnp.float32)
        precond, image, gram = pl.pallas_call(
            unpack_kernel,
            out_shape=(shard, shard, jax.ShapeDtypeStruct((KRYLOV + 1,), jnp.float32)),
            out_specs=(vmem, vmem, pl.BlockSpec(memory_space=pltpu.SMEM)),
            compiler_params=params,
            name="unpack",
        )(home, kept, tables)
        return precond, image, gram

    return jax.shard_map(
        on_device,
        mesh=mesh,
        in_specs=(P(None, "tm", "rows", None), P(None, None, "tm", "rows", None)),
        out_specs=(P(None, "tm", "rows", None), P(None, "tm", "rows", None), P()),
        check_vma=False,
    )
```

```python
import jax
import jax.numpy as jnp
import numpy as np
from jax import lax
from jax.experimental import pallas as pl
from jax.experimental.pallas import tpu as pltpu
from jax.sharding import PartitionSpec as P

ALPHA = 0.01
SWEEPS = 4
KRYLOV = 4
LANES = 128
ROWS = 8
SIDE = LANES // 2
MODES = 2 * ROWS
GROUP = 2 * MODES


def roll(value, amount, axis):
    size = value.shape[axis]
    return pltpu.roll(value, amount % size, axis)


def reversed_lanes(value):
    parts = [value[:, at : at + LANES] for at in range(0, value.shape[1], LANES)]
    index = LANES - 1 - lane_of(parts[0].shape)
    taken = [jnp.take_along_axis(p, index, axis=1, mode="promise_in_bounds") for p in parts]
    return jnp.concatenate(taken[::-1], 1)


def lane_of(shape):
    return lax.broadcasted_iota(jnp.int32, shape, len(shape) - 1)


def row_of(shape):
    return lax.broadcasted_iota(jnp.int32, shape, 0)


def sines(number, place, length):
    turn = np.outer(number, place + 1.0) / (length + 1)
    return np.sqrt(2.0 / (length + 1)) * np.sin(np.pi * turn)


def coupling(steps):
    return 16.0 / (steps * steps)


def time_table(steps):
    kappa = coupling(steps)
    index = np.arange(steps)
    gamma = ALPHA ** (index / steps)
    lam = 1.0 - ALPHA ** (1.0 / steps) * np.exp(-2j * np.pi * index / steps)
    den = lam * lam + 4.0 * kappa
    turn = np.exp(-2j * np.pi * np.outer(index, index) / steps)
    tables = []
    for m in range(SWEEPS):
        inner = np.conj(turn) @ ((1.0 / den ** (m + 1))[:, None] * turn) / steps
        tables.append(kappa**m * (inner.real / gamma[:, None]) * gamma[None, :])
    return np.concatenate(tables, 1)


def sine(turns, half):
    left = turns - jnp.floor(turns * (0.5 / half)) * (2.0 * half) - half
    near = jnp.abs(left)
    angle = jnp.minimum(near, half - near) * (np.pi / half)
    square = angle * angle
    series = jnp.full_like(square, -2.3889859e-8)
    for term in (2.7525562e-6, -1.9840874e-4, 8.3333310e-3, -1.6666667e-1, 1.0):
        series = series * square + term
    value = angle * series
    return jnp.where(left < 0.0, value, -value)


def column_table(half, dc):
    shape = (half, half)
    number = (2 * row_of(shape) + 1 + dc).astype(jnp.float32)
    place = (lane_of(shape) + 1).astype(jnp.float32)
    length = 2.0 * half + 1.0
    return sine(number * place, length) * np.sqrt(2.0 / length)


def symbol_of(block, cols):
    lane = lane_of((1, LANES))
    number = (2 * block + 1 + lane % GROUP // MODES).astype(jnp.float32)
    mode = (lane % MODES + 1).astype(jnp.float32)
    length, height = cols + 1.0, MODES + 1.0
    return 2.0 * (sine(number + 0.5 * length, length) + sine(mode + 0.5 * height, height))


def row_tables():
    wave = sines(np.arange(MODES) + 1, np.arange(MODES), MODES)
    enter = np.zeros((2, LANES, LANES))
    leave = np.zeros((LANES, 2, 2, LANES))
    for h in range(2):
        for row in range(ROWS):
            for dc in range(2):
                value = wave[:, h * ROWS + row]
                modes = dc * MODES + np.arange(MODES)
                for group in range(0, LANES, GROUP):
                    for c in range(2):
                        enter[h, dc * SIDE + c * ROWS + row, group + modes] = value
                for field, group in enumerate((0, 2, 1, 3)):
                    leave[group * GROUP + modes, 0, h, dc * SIDE + field * ROWS + row] = value
                for slot in (1, *range(KRYLOV, 2 * KRYLOV)):
                    leave[GROUP + modes, 1, h, dc * SIDE + slot * ROWS + row] = value
    enter = enter.reshape(4, SIDE, LANES).transpose(1, 0, 2).reshape(SIDE, 4 * LANES)
    return leave.reshape(LANES, 4 * LANES), enter


def halves(value):
    high = value.astype(jnp.bfloat16)
    return high, (value - high.astype(jnp.float32)).astype(jnp.bfloat16)


def both_halves(table):
    high = table.astype(jnp.bfloat16)
    return jnp.asarray(np.stack([high, (table - high.astype(np.float64)).astype(jnp.bfloat16)]))


def dot(left, right, contract):
    return lax.dot_general(left, right, (contract, ((), ())), preferred_element_type=jnp.float32)


def product(left, right, contract=((1,), (0,))):
    rows = left[0].shape[0]
    both = dot(jnp.concatenate([left[0], left[1]], 0), right[0], contract)
    return both[:rows] + (both[rows:] + dot(left[0], right[1], contract))


def folded(flat, basis, lent, second):
    half = flat.shape[1] // 2
    mixed = [jnp.where(second, lent[i], basis[i, 0]) for i in range(2)]
    whole = jnp.concatenate([flat] + mixed + [basis[i, 1] for i in range(KRYLOV)], 0)
    left, right = whole[:, :half], reversed_lanes(whole[:, half:])
    return [halves(left + right), halves(left - right)]


def turned_to_modes(fold, table):
    return product(table, fold, ((1,), (1,)))


def own_products(flat, basis):
    disp, velo = flat[:ROWS], flat[ROWS:]
    terms = [basis[i, 0] * disp + basis[i, 1] * velo for i in range(KRYLOV)]
    terms.append(disp * disp + velo * velo)
    sums = [sum(t[:, at : at + LANES] for at in range(0, t.shape[1], LANES)) for t in terms]
    return jnp.concatenate(sums, 0)


def delayed(value):
    moved = roll(value, 1, 0)
    return jnp.where(row_of(value.shape) == 0, ALPHA * moved, moved)


def solved(parts, own, symbol, time, enter, leave, kappa, count):
    steps = parts[0].shape[0]
    shape = (steps, LANES)
    lane, row = lane_of(shape), row_of(shape)
    is_disp = lane % SIDE < ROWS
    mixed = [jnp.where(is_disp, x - delayed(x), x) for x in parts]
    source = product(halves(jnp.concatenate(mixed, 1)), enter)
    line = lane_of((1, LANES))
    cut = line // GROUP == 1
    power, weights = jnp.ones((1, LANES), jnp.float32), []
    for m in range(SWEEPS):
        last = -kappa * power * symbol if m == SWEEPS - 1 else 0.0
        weights.append(jnp.where(cut, last, power))
        power = power * symbol
    stack = jnp.concatenate([source * weight for weight in weights], 0)
    found = product(time, halves(stack))
    late = delayed(found)
    group = lane // GROUP
    found = jnp.where(group == 2, found - late, found)
    found = jnp.where(group == 3, jnp.where(row == 0, late, 0.0), found)
    spread = product(halves(found), leave)
    at = line % SIDE
    slot = at // ROWS
    outs, gram, square = [], 0.0, 0.0
    for h, x in enumerate(parts):
        out = spread[:, h * LANES : (h + 1) * LANES]
        gone = spread[:, (2 + h) * LANES : (3 + h) * LANES]
        ended = roll(out[steps - 1 :], ROWS, 1) - roll(x[steps - 1 :], 2 * ROWS, 1)
        rate = jnp.where(slot == 2, ALPHA * ended, 0.0)
        outs.append(jnp.where((row == 0) & (slot == 2), out + rate, out))
        disp = jnp.where(slot == 3, out[:1], 0.0)
        inner = jnp.sum(jnp.where(slot >= KRYLOV, x * gone, gone * (2.0 * x + gone)), 0, keepdims=True)
        wide = roll(rate, 2 * ROWS, 1) + roll(rate, 3 * ROWS, 1)
        wide = wide + roll(wide, 2 * ROWS, 1)
        tail = roll(disp, -ROWS, 1) + disp
        gram = gram + jnp.where(slot >= KRYLOV, inner + x[:1] * wide, 0.0)
        gram = gram + jnp.where((slot == 4) | (slot == 5), roll(x[:1] * tail, 2 * ROWS, 1), 0.0)
        gram = gram + jnp.where((slot == 6) | (slot == 7), roll(x[1:2] * tail, 4 * ROWS, 1), 0.0)
        rate, disp = roll(rate, -ROWS, 1), roll(disp, -3 * ROWS, 1)
        square = square + jnp.where(slot == 1, inner + rate * (2.0 * (x[:1] + gone[:1]) + rate), 0.0)
        square = square + jnp.where(slot == 0, disp * (2.0 * x[:1] + disp), 0.0)
    totals = [
        jnp.sum(jnp.sum(own[i * ROWS : (i + 1) * ROWS], 0, keepdims=True), 1, keepdims=True)
        for i in range(KRYLOV + 1)
    ]
    extra = jnp.where(line == SIDE + GROUP, totals[KRYLOV] * (1.0 / count), 0.0)
    for i in range(KRYLOV):
        extra = extra + jnp.where(line == GROUP + i * ROWS, totals[i], 0.0)
    square = square * (1.0 / count)
    square = roll(square, GROUP + SIDE, 1) + roll(square, GROUP, 1)
    gram = jnp.where(line < SIDE, gram + roll(gram, SIDE, 1), square) + extra
    return [jnp.where(lane % SIDE >= GROUP, jnp.broadcast_to(gram, shape), out) for out in outs]


def gram_of(totals):
    line = lane_of(totals.shape)
    masks = [line // ROWS == GROUP // ROWS + i for i in range(KRYLOV)]
    masks.append(line // MODES == (SIDE + GROUP) // MODES)
    return [jnp.sum(jnp.where(mask, totals, 0.0)) for mask in masks]


def unpacked(received, flat, tables):
    turned = received.T
    sides = []
    for dc in range(2):
        fields = turned[dc * SIDE : dc * SIDE + GROUP]
        sides.append(product(halves(fields), tables[dc]))
    whole = jnp.concatenate([sides[0] + sides[1], reversed_lanes(sides[0] - sides[1])], 1)
    disp, rate, cut, edge = [whole[i * ROWS : (i + 1) * ROWS] for i in range(4)]
    return disp, rate - flat[:ROWS], flat[:ROWS] + edge, flat[ROWS:] + cut


def device_index():
    return lax.axis_index("tm") * 2 + lax.axis_index("rows")


def pack_kernel(
    resid_hbm, basis_hbm, later_hbm, lent_ref,
    send_ref, own_ref, resid_ref, tables_ref, later_ref, basis_ref, sems,
):
    pairs = ((resid_hbm, resid_ref), (basis_hbm, basis_ref), (later_hbm, later_ref))
    copies = [pltpu.make_async_copy(a, b, sems.at[i]) for i, (a, b) in enumerate(pairs)]
    for copy in copies:
        copy.start()
    second = lax.axis_index("tm") == 1
    tables = []
    for dc in range(2):
        tables.append(halves(column_table(tables_ref.shape[2], dc)))
        for part in range(2):
            tables_ref[dc, part] = tables[dc][part]
    for copy in copies[:2]:
        copy.wait()
    flat = resid_ref[...].reshape(MODES, resid_ref.shape[-1])
    basis = basis_ref[:, :, 0]
    folds = folded(flat, basis, lent_ref[2:, 0, 0], second)
    own_ref[...] = own_products(flat, basis)
    sides = [turned_to_modes(folds[dc], tables_ref[dc]) for dc in range(2)]
    send_ref[...] = jnp.concatenate(sides, 1)
    copies[2].wait()


def solve_kernel(
    kappa, count, steps, cols, recv_ref, own_ref, tables_ref, send_ref
):
    time, leave = tables_ref[:, :steps], tables_ref[:, steps : steps + LANES]
    stored = tables_ref[:, steps + LANES :]
    enter = jnp.concatenate([stored[:, :, at : at + LANES] for at in range(0, 4 * LANES, LANES)], 1)
    parts = [recv_ref[pl.ds(h, steps, stride=2), :] for h in range(2)]
    outs = solved(
        parts, own_ref[...], symbol_of(device_index(), cols), time, enter, leave, kappa, count
    )
    for h, out in enumerate(outs):
        send_ref[pl.ds(h, steps, stride=2), :] = out


def unpack_kernel(recv_ref, resid_ref, tables_ref, precond_ref, image_ref, gram_ref):
    received = recv_ref[...]
    flat = resid_ref[...].reshape(MODES, resid_ref.shape[-1])
    for slot, field in enumerate(unpacked(received, flat, tables_ref)):
        (precond_ref, image_ref)[slot // 2][slot % 2, 0] = field
    for i, value in enumerate(gram_of(jnp.sum(received, 0, keepdims=True))):
        gram_ref[i] = value


def solution(mesh):
    axes = ("tm", "rows")
    steps = mesh.shape["tm"]
    devices = steps * mesh.shape["rows"]
    params = pltpu.CompilerParams(vmem_limit_bytes=12 * 2**20)

    def on_device(resid, basis):
        cols = resid.shape[3]
        kappa = coupling(steps)
        count = 2.0 * steps * MODES * cols
        solve_tables = both_halves(np.concatenate([time_table(steps), *row_tables()], 0))
        vmem = pl.BlockSpec(memory_space=pltpu.VMEM)
        hbm = pl.BlockSpec(memory_space=pltpu.HBM)
        placed = [pltpu.with_memory_space_constraint(a, pltpu.HBM) for a in (resid, basis, solve_tables)]
        message = jax.ShapeDtypeStruct((devices, LANES), jnp.float32)
        lent = lax.ppermute(basis, "tm", [(0, 1)])
        send, own, kept, tables, solve_tables = pl.pallas_call(
            pack_kernel,
            in_specs=[hbm, hbm, hbm, vmem],
            out_shape=(
                message,
                jax.ShapeDtypeStruct(((KRYLOV + 1) * ROWS, LANES), jnp.float32),
                jax.ShapeDtypeStruct(resid.shape, jnp.float32),
                jax.ShapeDtypeStruct((2, 2, cols // 2, cols // 2), jnp.bfloat16),
                jax.ShapeDtypeStruct(solve_tables.shape, jnp.bfloat16),
            ),
            scratch_shapes=[
                pltpu.VMEM(basis.shape, jnp.float32),
                pltpu.SemaphoreType.DMA((3,)),
            ],
            compiler_params=params,
            name="pack",
        )(*placed, lent)
        recv = lax.all_to_all(send, axes, 0, 0, tiled=True)
        back = pl.pallas_call(
            lambda *refs: solve_kernel(kappa, count, steps, cols, *refs),
            out_shape=message,
            compiler_params=params,
            name="solve",
        )(recv, own, solve_tables)
        home = lax.all_to_all(back, axes, 0, 0, tiled=True)
        shard = jax.ShapeDtypeStruct(resid.shape, jnp.float32)
        precond, image, gram = pl.pallas_call(
            unpack_kernel,
            out_shape=(shard, shard, jax.ShapeDtypeStruct((KRYLOV + 1,), jnp.float32)),
            out_specs=(vmem, vmem, pl.BlockSpec(memory_space=pltpu.SMEM)),
            compiler_params=params,
            name="unpack",
        )(home, kept, tables)
        return precond, image, gram

    return jax.shard_map(
        on_device,
        mesh=mesh,
        in_specs=(P(None, "tm", "rows", None), P(None, None, "tm", "rows", None)),
        out_specs=(P(None, "tm", "rows", None), P(None, "tm", "rows", None), P()),
        check_vma=False,
    )
```

```python
import jax
import jax.numpy as jnp
import numpy as np
from jax import lax
from jax.experimental import pallas as pl
from jax.experimental.pallas import tpu as pltpu
from jax.sharding import PartitionSpec as P

ALPHA = 0.01
SWEEPS = 4
KRYLOV = 4
LANES = 128
ROWS = 8
SIDE = LANES // 2
MODES = 2 * ROWS
GROUP = 2 * MODES


def roll(value, amount, axis):
    size = value.shape[axis]
    return pltpu.roll(value, amount % size, axis)


def reversed_lanes(value):
    parts = [value[:, at : at + LANES] for at in range(0, value.shape[1], LANES)]
    index = LANES - 1 - lane_of(parts[0].shape)
    taken = [jnp.take_along_axis(p, index, axis=1, mode="promise_in_bounds") for p in parts]
    return jnp.concatenate(taken[::-1], 1)


def lane_of(shape):
    return lax.broadcasted_iota(jnp.int32, shape, len(shape) - 1)


def row_of(shape):
    return lax.broadcasted_iota(jnp.int32, shape, 0)


def sines(number, place, length):
    turn = np.outer(number, place + 1.0) / (length + 1)
    return np.sqrt(2.0 / (length + 1)) * np.sin(np.pi * turn)


def coupling(steps):
    return 16.0 / (steps * steps)


def time_table(steps):
    kappa = coupling(steps)
    index = np.arange(steps)
    gamma = ALPHA ** (index / steps)
    lam = 1.0 - ALPHA ** (1.0 / steps) * np.exp(-2j * np.pi * index / steps)
    den = lam * lam + 4.0 * kappa
    turn = np.exp(-2j * np.pi * np.outer(index, index) / steps)
    tables = []
    for m in range(SWEEPS):
        inner = np.conj(turn) @ ((1.0 / den ** (m + 1))[:, None] * turn) / steps
        tables.append(kappa**m * (inner.real / gamma[:, None]) * gamma[None, :])
    return np.concatenate(tables, 1)


def sine(turns, half):
    left = turns - jnp.floor(turns * (0.5 / half)) * (2.0 * half) - half
    near = jnp.abs(left)
    angle = jnp.minimum(near, half - near) * (np.pi / half)
    square = angle * angle
    series = jnp.full_like(square, -2.3889859e-8)
    for term in (2.7525562e-6, -1.9840874e-4, 8.3333310e-3, -1.6666667e-1, 1.0):
        series = series * square + term
    value = angle * series
    return jnp.where(left < 0.0, value, -value)


def column_table(half, dc):
    shape = (half, half)
    number = (2 * row_of(shape) + 1 + dc).astype(jnp.float32)
    place = (lane_of(shape) + 1).astype(jnp.float32)
    length = 2.0 * half + 1.0
    return sine(number * place, length) * np.sqrt(2.0 / length)


def symbol_of(block, cols):
    lane = lane_of((1, LANES))
    number = (2 * block + 1 + lane % GROUP // MODES).astype(jnp.float32)
    mode = (lane % MODES + 1).astype(jnp.float32)
    length, height = cols + 1.0, MODES + 1.0
    return 2.0 * (sine(number + 0.5 * length, length) + sine(mode + 0.5 * height, height))


def row_tables():
    wave = sines(np.arange(MODES) + 1, np.arange(MODES), MODES)
    enter = np.zeros((2, LANES, GROUP))
    leave = np.zeros((LANES, 2, 2, LANES))
    for h in range(2):
        for row in range(ROWS):
            for dc in range(2):
                value = wave[:, h * ROWS + row]
                modes = dc * MODES + np.arange(MODES)
                enter[h, dc * SIDE + ROWS + row, modes] = value
                for field, group in enumerate((0, 2, 1, 3)):
                    leave[group * GROUP + modes, 0, h, dc * SIDE + field * ROWS + row] = value
                for slot in (1, *range(KRYLOV, 2 * KRYLOV)):
                    leave[GROUP + modes, 1, h, dc * SIDE + slot * ROWS + row] = value
    return enter.reshape(2 * LANES, GROUP), leave.reshape(LANES, 4 * LANES)


def cut_up(table, count):
    pieces = []
    for _ in range(count):
        pieces.append(table.astype(jnp.bfloat16))
        table = table - pieces[-1].astype(np.float64)
    return pieces


def solve_constants(steps):
    enter, leave = row_tables()
    pieces = cut_up(enter, 3)
    enter = np.concatenate([*pieces, np.zeros_like(pieces[0])], 1)
    enter = enter.reshape(4, SIDE, LANES).transpose(1, 0, 2).reshape(SIDE, 4 * LANES)
    rows = [*cut_up(time_table(steps), 3), *cut_up(leave, 2), enter]
    return jnp.asarray(np.concatenate(rows, 0))


def halves(value):
    high = value.astype(jnp.bfloat16)
    return high, (value - high.astype(jnp.float32)).astype(jnp.bfloat16)


def thirds(value):
    high, low = halves(value)
    rest = value - high.astype(jnp.float32) - low.astype(jnp.float32)
    return high, low, rest.astype(jnp.bfloat16)


def third_by_group(value):
    group = lane_of(value.shape) // GROUP
    first = value - value.astype(jnp.bfloat16).astype(jnp.float32)
    second = first - first.astype(jnp.bfloat16).astype(jnp.float32)
    chosen = jnp.where(group == 0, value, jnp.where(group == 1, first, second))
    return jnp.where(group == 3, 0.0, chosen).astype(jnp.bfloat16)


def groups_added(value):
    value = value + roll(value, 2 * GROUP, 1)
    return value + roll(value, GROUP, 1)


def thirds_added(value):
    rows = value.shape[0] // 3
    return value[:rows] + (value[rows : 2 * rows] + value[2 * rows :])


def dot(left, right, contract):
    return lax.dot_general(left, right, (contract, ((), ())), preferred_element_type=jnp.float32)


def product(left, right, contract=((1,), (0,))):
    rows = left[0].shape[0]
    both = dot(jnp.concatenate([left[0], left[1]], 0), right[0], contract)
    return both[:rows] + (both[rows:] + dot(left[0], right[1], contract))


def folded(flat, basis, lent, second):
    half = flat.shape[1] // 2
    mixed = [jnp.where(second, lent[i], basis[i, 0]) for i in range(2)]
    whole = jnp.concatenate([flat] + mixed + [basis[i, 1] for i in range(KRYLOV)], 0)
    left, right = whole[:, :half], reversed_lanes(whole[:, half:])
    return [left + right, left - right]


def turned_to_modes(folds, tables):
    turned = []
    for fold, table in zip(folds, tables):
        pieces = jnp.concatenate([*thirds(fold), jnp.zeros(fold.shape, jnp.bfloat16)], 0)
        half = table.shape[1]
        parts = dot(table.reshape(2 * half, half), pieces, ((1,), (1,)))
        parts = parts[:half] + parts[half:]
        parts = parts[:, :LANES] + parts[:, LANES:]
        turned.append(parts + roll(parts, SIDE, 1))
    return jnp.where(lane_of(turned[0].shape) < SIDE, *turned)


def own_products(flat, basis):
    disp, velo = flat[:ROWS], flat[ROWS:]
    terms = [basis[i, 0] * disp + basis[i, 1] * velo for i in range(KRYLOV)]
    terms.append(disp * disp + velo * velo)
    sums = [sum(t[:, at : at + LANES] for at in range(0, t.shape[1], LANES)) for t in terms]
    return jnp.concatenate(sums, 0)


def delayed(value):
    moved = roll(value, 1, 0)
    return jnp.where(row_of(value.shape) == 0, ALPHA * moved, moved)


def solved(parts, own, symbol, time, enter, leave, kappa, count):
    steps = parts[0].shape[0]
    shape = (steps, LANES)
    lane, row = lane_of(shape), row_of(shape)
    is_velo = lane % SIDE // ROWS == 1
    mixed = [jnp.where(is_velo, x + roll(x - delayed(x), ROWS, 1), 0.0) for x in parts]
    pieces = jnp.concatenate(thirds(jnp.concatenate(mixed, 1)), 0)
    source = groups_added(thirds_added(dot(pieces, enter, ((1,), (0,)))))
    line = lane_of((1, LANES))
    power, stack = jnp.ones((1, LANES), jnp.float32), []
    for m in range(SWEEPS):
        stack.append(third_by_group(source * power))
        power = power * symbol
    blank = jnp.zeros(((SWEEPS - 1) * steps, LANES), jnp.bfloat16)
    last = jnp.concatenate([blank, third_by_group(source * (-kappa * power))], 0)
    stack = jnp.concatenate([jnp.concatenate(stack, 0), last], 1)
    found = thirds_added(dot(time, stack, ((1,), (0,))))
    gone = groups_added(found[:, LANES:])
    found = groups_added(found[:, :LANES])
    late = delayed(found)
    group = lane // GROUP
    found = jnp.where(group == 1, gone, jnp.where(group == 2, found - late, found))
    found = jnp.where(group == 3, jnp.where(row == 0, late, 0.0), found)
    spread = product(halves(found), leave)
    at = line % SIDE
    slot = at // ROWS
    outs, gram, square = [], 0.0, 0.0
    for h, x in enumerate(parts):
        out = spread[:, h * LANES : (h + 1) * LANES]
        gone = spread[:, (2 + h) * LANES : (3 + h) * LANES]
        ended = roll(out[steps - 1 :], ROWS, 1) - roll(x[steps - 1 :], 2 * ROWS, 1)
        rate = jnp.where(slot == 2, ALPHA * ended, 0.0)
        outs.append(jnp.where((row == 0) & (slot == 2), out + rate, out))
        disp = jnp.where(slot == 3, out[:1], 0.0)
        inner = jnp.sum(jnp.where(slot >= KRYLOV, x * gone, gone * (2.0 * x + gone)), 0, keepdims=True)
        wide = roll(rate, 2 * ROWS, 1) + roll(rate, 3 * ROWS, 1)
        wide = wide + roll(wide, 2 * ROWS, 1)
        tail = roll(disp, -ROWS, 1) + disp
        gram = gram + jnp.where(slot >= KRYLOV, inner + x[:1] * wide, 0.0)
        gram = gram + jnp.where((slot == 4) | (slot == 5), roll(x[:1] * tail, 2 * ROWS, 1), 0.0)
        gram = gram + jnp.where((slot == 6) | (slot == 7), roll(x[1:2] * tail, 4 * ROWS, 1), 0.0)
        rate, disp = roll(rate, -ROWS, 1), roll(disp, -3 * ROWS, 1)
        square = square + jnp.where(slot == 1, inner + rate * (2.0 * (x[:1] + gone[:1]) + rate), 0.0)
        square = square + jnp.where(slot == 0, disp * (2.0 * x[:1] + disp), 0.0)
    totals = [
        jnp.sum(jnp.sum(own[i * ROWS : (i + 1) * ROWS], 0, keepdims=True), 1, keepdims=True)
        for i in range(KRYLOV + 1)
    ]
    extra = jnp.where(line == SIDE + GROUP, totals[KRYLOV] * (1.0 / count), 0.0)
    for i in range(KRYLOV):
        extra = extra + jnp.where(line == GROUP + i * ROWS, totals[i], 0.0)
    square = square * (1.0 / count)
    square = roll(square, GROUP + SIDE, 1) + roll(square, GROUP, 1)
    gram = jnp.where(line < SIDE, gram + roll(gram, SIDE, 1), square) + extra
    return [jnp.where(lane % SIDE >= GROUP, jnp.broadcast_to(gram, shape), out) for out in outs]


def gram_of(totals):
    line = lane_of(totals.shape)
    masks = [line // ROWS == GROUP // ROWS + i for i in range(KRYLOV)]
    masks.append(line // MODES == (SIDE + GROUP) // MODES)
    return [jnp.sum(jnp.where(mask, totals, 0.0)) for mask in masks]


def unpacked(received, flat, tables):
    turned = received.T
    sides = []
    for dc in range(2):
        fields = turned[dc * SIDE : dc * SIDE + GROUP]
        sides.append(product(halves(fields), tables[dc]))
    whole = jnp.concatenate([sides[0] + sides[1], reversed_lanes(sides[0] - sides[1])], 1)
    disp, rate, cut, edge = [whole[i * ROWS : (i + 1) * ROWS] for i in range(4)]
    return disp, rate - flat[:ROWS], flat[:ROWS] + edge, flat[ROWS:] + cut


def device_index():
    return lax.axis_index("tm") * 2 + lax.axis_index("rows")


def pack_kernel(
    resid_hbm, basis_hbm, later_hbm, lent_ref,
    send_ref, own_ref, resid_ref, tables_ref, later_ref, basis_ref, sems,
):
    pairs = ((resid_hbm, resid_ref), (basis_hbm, basis_ref), (later_hbm, later_ref))
    copies = [pltpu.make_async_copy(a, b, sems.at[i]) for i, (a, b) in enumerate(pairs)]
    for copy in copies:
        copy.start()
    second = lax.axis_index("tm") == 1
    for dc in range(2):
        for part, table in enumerate(halves(column_table(tables_ref.shape[2], dc))):
            tables_ref[dc, part] = table
    for copy in copies[:2]:
        copy.wait()
    flat = resid_ref[...].reshape(MODES, resid_ref.shape[-1])
    basis = basis_ref[:, :, 0]
    folds = folded(flat, basis, lent_ref[2:, 0, 0], second)
    own_ref[...] = own_products(flat, basis)
    send_ref[...] = turned_to_modes(folds, [tables_ref[dc] for dc in range(2)])
    copies[2].wait()


def solve_kernel(
    kappa, count, steps, cols, recv_ref, own_ref, tables_ref, send_ref
):
    time = tables_ref[: 3 * steps]
    leave = [tables_ref[at : at + LANES] for at in (3 * steps, 3 * steps + LANES)]
    stored = tables_ref[3 * steps + 2 * LANES :]
    enter = jnp.concatenate([stored[:, at : at + LANES] for at in range(0, 4 * LANES, LANES)], 0)
    parts = [recv_ref[pl.ds(h, steps, stride=2), :] for h in range(2)]
    outs = solved(
        parts, own_ref[...], symbol_of(device_index(), cols), time, enter, leave, kappa, count
    )
    for h, out in enumerate(outs):
        send_ref[pl.ds(h, steps, stride=2), :] = out


def unpack_kernel(recv_ref, resid_ref, tables_ref, precond_ref, image_ref, gram_ref):
    received = recv_ref[...]
    flat = resid_ref[...].reshape(MODES, resid_ref.shape[-1])
    for slot, field in enumerate(unpacked(received, flat, tables_ref)):
        (precond_ref, image_ref)[slot // 2][slot % 2, 0] = field
    for i, value in enumerate(gram_of(jnp.sum(received, 0, keepdims=True))):
        gram_ref[i] = value


def solution(mesh):
    axes = ("tm", "rows")
    steps = mesh.shape["tm"]
    devices = steps * mesh.shape["rows"]
    params = pltpu.CompilerParams(vmem_limit_bytes=12 * 2**20)

    def on_device(resid, basis):
        cols = resid.shape[3]
        kappa = coupling(steps)
        count = 2.0 * steps * MODES * cols
        solve_tables = solve_constants(steps)
        vmem = pl.BlockSpec(memory_space=pltpu.VMEM)
        hbm = pl.BlockSpec(memory_space=pltpu.HBM)
        placed = [pltpu.with_memory_space_constraint(a, pltpu.HBM) for a in (resid, basis, solve_tables)]
        message = jax.ShapeDtypeStruct((devices, LANES), jnp.float32)
        lent = lax.ppermute(basis, "tm", [(0, 1)])
        send, own, kept, tables, solve_tables = pl.pallas_call(
            pack_kernel,
            in_specs=[hbm, hbm, hbm, vmem],
            out_shape=(
                message,
                jax.ShapeDtypeStruct(((KRYLOV + 1) * ROWS, LANES), jnp.float32),
                jax.ShapeDtypeStruct(resid.shape, jnp.float32),
                jax.ShapeDtypeStruct((2, 2, cols // 2, cols // 2), jnp.bfloat16),
                jax.ShapeDtypeStruct(solve_tables.shape, jnp.bfloat16),
            ),
            scratch_shapes=[
                pltpu.VMEM(basis.shape, jnp.float32),
                pltpu.SemaphoreType.DMA((3,)),
            ],
            compiler_params=params,
            name="pack",
        )(*placed, lent)
        recv = lax.all_to_all(send, axes, 0, 0, tiled=True)
        back = pl.pallas_call(
            lambda *refs: solve_kernel(kappa, count, steps, cols, *refs),
            out_shape=message,
            compiler_params=params,
            name="solve",
        )(recv, own, solve_tables)
        home = lax.all_to_all(back, axes, 0, 0, tiled=True)
        shard = jax.ShapeDtypeStruct(resid.shape, jnp.float32)
        precond, image, gram = pl.pallas_call(
            unpack_kernel,
            out_shape=(shard, shard, jax.ShapeDtypeStruct((KRYLOV + 1,), jnp.float32)),
            out_specs=(vmem, vmem, pl.BlockSpec(memory_space=pltpu.SMEM)),
            compiler_params=params,
            name="unpack",
        )(home, kept, tables)
        return precond, image, gram

    return jax.shard_map(
        on_device,
        mesh=mesh,
        in_specs=(P(None, "tm", "rows", None), P(None, None, "tm", "rows", None)),
        out_specs=(P(None, "tm", "rows", None), P(None, "tm", "rows", None), P()),
        check_vma=False,
    )
```

```python
import jax
import jax.numpy as jnp
import numpy as np
from jax import lax
from jax.experimental import pallas as pl
from jax.experimental.pallas import tpu as pltpu
from jax.sharding import PartitionSpec as P

ALPHA = 0.01
SWEEPS = 4
KRYLOV = 4
LANES = 128
ROWS = 8
SIDE = LANES // 2
MODES = 2 * ROWS
GROUP = 2 * MODES


def roll(value, amount, axis):
    size = value.shape[axis]
    return pltpu.roll(value, amount % size, axis)


def reversed_lanes(value):
    parts = [value[:, at : at + LANES] for at in range(0, value.shape[1], LANES)]
    index = LANES - 1 - lane_of(parts[0].shape)
    taken = [jnp.take_along_axis(p, index, axis=1, mode="promise_in_bounds") for p in parts]
    return jnp.concatenate(taken[::-1], 1)


def lane_of(shape):
    return lax.broadcasted_iota(jnp.int32, shape, len(shape) - 1)


def row_of(shape):
    return lax.broadcasted_iota(jnp.int32, shape, 0)


def sines(number, place, length):
    turn = np.outer(number, place + 1.0) / (length + 1)
    return np.sqrt(2.0 / (length + 1)) * np.sin(np.pi * turn)


def coupling(steps):
    return 16.0 / (steps * steps)


def time_table(steps):
    kappa = coupling(steps)
    index = np.arange(steps)
    gamma = ALPHA ** (index / steps)
    lam = 1.0 - ALPHA ** (1.0 / steps) * np.exp(-2j * np.pi * index / steps)
    den = lam * lam + 4.0 * kappa
    turn = np.exp(-2j * np.pi * np.outer(index, index) / steps)
    tables = []
    for m in range(SWEEPS):
        inner = np.conj(turn) @ ((1.0 / den ** (m + 1))[:, None] * turn) / steps
        tables.append(kappa**m * (inner.real / gamma[:, None]) * gamma[None, :])
    return np.concatenate(tables, 1)


def sine(turns, half):
    left = turns - jnp.floor(turns * (0.5 / half)) * (2.0 * half) - half
    near = jnp.abs(left)
    angle = jnp.minimum(near, half - near) * (np.pi / half)
    square = angle * angle
    series = jnp.full_like(square, -2.3889859e-8)
    for term in (2.7525562e-6, -1.9840874e-4, 8.3333310e-3, -1.6666667e-1, 1.0):
        series = series * square + term
    value = angle * series
    return jnp.where(left < 0.0, value, -value)


def column_table(half, dc):
    shape = (half, half)
    number = (2 * row_of(shape) + 1 + dc).astype(jnp.float32)
    place = (lane_of(shape) + 1).astype(jnp.float32)
    length = 2.0 * half + 1.0
    return sine(number * place, length) * np.sqrt(2.0 / length)


def symbol_of(block, cols):
    lane = lane_of((1, LANES))
    number = (2 * block + 1 + lane % GROUP // MODES).astype(jnp.float32)
    mode = (lane % MODES + 1).astype(jnp.float32)
    length, height = cols + 1.0, MODES + 1.0
    return 2.0 * (sine(number + 0.5 * length, length) + sine(mode + 0.5 * height, height))


def row_tables():
    wave = sines(np.arange(MODES) + 1, np.arange(MODES), MODES)
    enter = np.zeros((2, LANES, GROUP))
    leave = np.zeros((LANES, 2, 2, LANES))
    for h in range(2):
        for row in range(ROWS):
            for dc in range(2):
                value = wave[:, h * ROWS + row]
                modes = dc * MODES + np.arange(MODES)
                enter[h, dc * SIDE + ROWS + row, modes] = value
                for field, group in enumerate((0, 2, 1, 3)):
                    leave[group * GROUP + modes, 0, h, dc * SIDE + field * ROWS + row] = value
                for slot in (1, *range(KRYLOV, 2 * KRYLOV)):
                    leave[GROUP + modes, 1, h, dc * SIDE + slot * ROWS + row] = value
    return enter.reshape(2 * LANES, GROUP), leave.reshape(LANES, 4 * LANES)


def cut_up(table, count):
    pieces = []
    for _ in range(count):
        pieces.append(table.astype(jnp.bfloat16))
        table = table - pieces[-1].astype(np.float64)
    return pieces


def solve_constants(steps):
    enter, leave = row_tables()
    pieces = cut_up(enter, 3)
    enter = np.concatenate([*pieces, np.zeros_like(pieces[0])], 1)
    enter = enter.reshape(4, SIDE, LANES).transpose(1, 0, 2).reshape(SIDE, 4 * LANES)
    rows = [*cut_up(time_table(steps), 3), *cut_up(leave, 2), enter]
    return jnp.asarray(np.concatenate(rows, 0))


def halves(value):
    high = value.astype(jnp.bfloat16)
    return high, (value - high.astype(jnp.float32)).astype(jnp.bfloat16)


def thirds(value):
    high, low = halves(value)
    rest = value - high.astype(jnp.float32) - low.astype(jnp.float32)
    return high, low, rest.astype(jnp.bfloat16)


def third_by_group(value):
    group = lane_of(value.shape) // GROUP
    first = value - value.astype(jnp.bfloat16).astype(jnp.float32)
    second = first - first.astype(jnp.bfloat16).astype(jnp.float32)
    chosen = jnp.where(group == 0, value, jnp.where(group == 1, first, second))
    return jnp.where(group == 3, 0.0, chosen).astype(jnp.bfloat16)


def groups_added(value):
    value = value + roll(value, 2 * GROUP, 1)
    return value + roll(value, GROUP, 1)


def thirds_added(value):
    rows = value.shape[0] // 3
    return value[:rows] + (value[rows : 2 * rows] + value[2 * rows :])


def dot(left, right, contract):
    return lax.dot_general(left, right, (contract, ((), ())), preferred_element_type=jnp.float32)


def product(left, right, contract=((1,), (0,))):
    rows = left[0].shape[0]
    both = dot(jnp.concatenate([left[0], left[1]], 0), right[0], contract)
    return both[:rows] + (both[rows:] + dot(left[0], right[1], contract))


def folded(flat, basis, lent, second):
    half = flat.shape[1] // 2
    mixed = [jnp.where(second, lent[i], basis[i, 0]) for i in range(2)]
    whole = jnp.concatenate([flat] + mixed + [basis[i, 1] for i in range(KRYLOV)], 0)
    left, right = whole[:, :half], reversed_lanes(whole[:, half:])
    return [left + right, left - right]


def turned_to_modes(folds, tables):
    turned = []
    for fold, table in zip(folds, tables):
        pieces = jnp.concatenate([*thirds(fold), jnp.zeros(fold.shape, jnp.bfloat16)], 0)
        half = table.shape[1]
        parts = dot(table.reshape(2 * half, half), pieces, ((1,), (1,)))
        parts = parts[:half] + parts[half:]
        parts = parts[:, :LANES] + parts[:, LANES:]
        turned.append(parts + roll(parts, SIDE, 1))
    return jnp.where(lane_of(turned[0].shape) < SIDE, *turned)


def own_products(flat, basis):
    disp, velo = flat[:ROWS], flat[ROWS:]
    terms = [basis[i, 0] * disp + basis[i, 1] * velo for i in range(KRYLOV)]
    terms.append(disp * disp + velo * velo)
    sums = [sum(t[:, at : at + LANES] for at in range(0, t.shape[1], LANES)) for t in terms]
    return jnp.concatenate(sums, 0)


def delayed(value):
    moved = roll(value, 1, 0)
    return jnp.where(row_of(value.shape) == 0, ALPHA * moved, moved)


def solved(parts, own, symbol, time, enter, leave, kappa, count):
    steps = parts[0].shape[0]
    shape = (steps, LANES)
    lane, row = lane_of(shape), row_of(shape)
    is_velo = lane % SIDE // ROWS == 1
    mixed = [jnp.where(is_velo, x + roll(x - delayed(x), ROWS, 1), 0.0) for x in parts]
    pieces = jnp.concatenate(thirds(jnp.concatenate(mixed, 1)), 0)
    source = groups_added(thirds_added(dot(pieces, enter, ((1,), (0,)))))
    line = lane_of((1, LANES))
    source = third_by_group(source)
    power, found = 1.0, 0.0
    for m in range(SWEEPS):
        part = dot(time[:, m * steps : (m + 1) * steps], source, ((1,), (0,)))
        part = thirds_added(part) * power
        found = found + part
        power = power * symbol
    gone = groups_added(part * (-kappa * symbol))
    found = groups_added(found)
    late = delayed(found)
    group = lane // GROUP
    found = jnp.where(group == 1, gone, jnp.where(group == 2, found - late, found))
    found = jnp.where(group == 3, jnp.where(row == 0, late, 0.0), found)
    spread = product(halves(found), leave)
    at = line % SIDE
    slot = at // ROWS
    outs, gram, square = [], 0.0, 0.0
    for h, x in enumerate(parts):
        out = spread[:, h * LANES : (h + 1) * LANES]
        gone = spread[:, (2 + h) * LANES : (3 + h) * LANES]
        ended = roll(out[steps - 1 :], ROWS, 1) - roll(x[steps - 1 :], 2 * ROWS, 1)
        rate = jnp.where(slot == 2, ALPHA * ended, 0.0)
        outs.append(jnp.where((row == 0) & (slot == 2), out + rate, out))
        disp = jnp.where(slot == 3, out[:1], 0.0)
        inner = jnp.sum(jnp.where(slot >= KRYLOV, x * gone, gone * (2.0 * x + gone)), 0, keepdims=True)
        wide = roll(rate, 2 * ROWS, 1) + roll(rate, 3 * ROWS, 1)
        wide = wide + roll(wide, 2 * ROWS, 1)
        tail = roll(disp, -ROWS, 1) + disp
        gram = gram + jnp.where(slot >= KRYLOV, inner + x[:1] * wide, 0.0)
        gram = gram + jnp.where((slot == 4) | (slot == 5), roll(x[:1] * tail, 2 * ROWS, 1), 0.0)
        gram = gram + jnp.where((slot == 6) | (slot == 7), roll(x[1:2] * tail, 4 * ROWS, 1), 0.0)
        rate, disp = roll(rate, -ROWS, 1), roll(disp, -3 * ROWS, 1)
        square = square + jnp.where(slot == 1, inner + rate * (2.0 * (x[:1] + gone[:1]) + rate), 0.0)
        square = square + jnp.where(slot == 0, disp * (2.0 * x[:1] + disp), 0.0)
    totals = [
        jnp.sum(jnp.sum(own[i * ROWS : (i + 1) * ROWS], 0, keepdims=True), 1, keepdims=True)
        for i in range(KRYLOV + 1)
    ]
    extra = jnp.where(line == SIDE + GROUP, totals[KRYLOV] * (1.0 / count), 0.0)
    for i in range(KRYLOV):
        extra = extra + jnp.where(line == GROUP + i * ROWS, totals[i], 0.0)
    square = square * (1.0 / count)
    square = roll(square, GROUP + SIDE, 1) + roll(square, GROUP, 1)
    gram = jnp.where(line < SIDE, gram + roll(gram, SIDE, 1), square) + extra
    return [jnp.where(lane % SIDE >= GROUP, jnp.broadcast_to(gram, shape), out) for out in outs]


def gram_of(totals):
    line = lane_of(totals.shape)
    masks = [line // ROWS == GROUP // ROWS + i for i in range(KRYLOV)]
    masks.append(line // MODES == (SIDE + GROUP) // MODES)
    return [jnp.sum(jnp.where(mask, totals, 0.0)) for mask in masks]


def unpacked(received, flat, tables):
    turned = received.T
    sides = []
    for dc in range(2):
        fields = turned[dc * SIDE : dc * SIDE + GROUP]
        sides.append(product(halves(fields), tables[dc]))
    whole = jnp.concatenate([sides[0] + sides[1], reversed_lanes(sides[0] - sides[1])], 1)
    disp, rate, cut, edge = [whole[i * ROWS : (i + 1) * ROWS] for i in range(4)]
    return disp, rate - flat[:ROWS], flat[:ROWS] + edge, flat[ROWS:] + cut


def device_index():
    return lax.axis_index("tm") * 2 + lax.axis_index("rows")


def pack_kernel(
    resid_hbm, basis_hbm, later_hbm, lent_ref,
    send_ref, own_ref, resid_ref, tables_ref, later_ref, basis_ref, sems,
):
    pairs = ((resid_hbm, resid_ref), (basis_hbm, basis_ref), (later_hbm, later_ref))
    copies = [pltpu.make_async_copy(a, b, sems.at[i]) for i, (a, b) in enumerate(pairs)]
    for copy in copies:
        copy.start()
    second = lax.axis_index("tm") == 1
    for dc in range(2):
        for part, table in enumerate(halves(column_table(tables_ref.shape[2], dc))):
            tables_ref[dc, part] = table
    for copy in copies[:2]:
        copy.wait()
    flat = resid_ref[...].reshape(MODES, resid_ref.shape[-1])
    basis = basis_ref[:, :, 0]
    folds = folded(flat, basis, lent_ref[2:, 0, 0], second)
    own_ref[...] = own_products(flat, basis)
    send_ref[...] = turned_to_modes(folds, [tables_ref[dc] for dc in range(2)])
    copies[2].wait()


def solve_kernel(
    kappa, count, steps, cols, recv_ref, own_ref, tables_ref, send_ref
):
    time = tables_ref[: 3 * steps]
    leave = [tables_ref[at : at + LANES] for at in (3 * steps, 3 * steps + LANES)]
    stored = tables_ref[3 * steps + 2 * LANES :]
    enter = jnp.concatenate([stored[:, at : at + LANES] for at in range(0, 4 * LANES, LANES)], 0)
    parts = [recv_ref[pl.ds(h, steps, stride=2), :] for h in range(2)]
    outs = solved(
        parts, own_ref[...], symbol_of(device_index(), cols), time, enter, leave, kappa, count
    )
    for h, out in enumerate(outs):
        send_ref[pl.ds(h, steps, stride=2), :] = out


def unpack_kernel(recv_ref, resid_ref, tables_ref, precond_ref, image_ref, gram_ref):
    received = recv_ref[...]
    flat = resid_ref[...].reshape(MODES, resid_ref.shape[-1])
    for slot, field in enumerate(unpacked(received, flat, tables_ref)):
        (precond_ref, image_ref)[slot // 2][slot % 2, 0] = field
    for i, value in enumerate(gram_of(jnp.sum(received, 0, keepdims=True))):
        gram_ref[i] = value


def solution(mesh):
    axes = ("tm", "rows")
    steps = mesh.shape["tm"]
    devices = steps * mesh.shape["rows"]
    params = pltpu.CompilerParams(vmem_limit_bytes=12 * 2**20)

    def on_device(resid, basis):
        cols = resid.shape[3]
        kappa = coupling(steps)
        count = 2.0 * steps * MODES * cols
        solve_tables = solve_constants(steps)
        vmem = pl.BlockSpec(memory_space=pltpu.VMEM)
        hbm = pl.BlockSpec(memory_space=pltpu.HBM)
        placed = [pltpu.with_memory_space_constraint(a, pltpu.HBM) for a in (resid, basis, solve_tables)]
        message = jax.ShapeDtypeStruct((devices, LANES), jnp.float32)
        lent = lax.ppermute(basis, "tm", [(0, 1)])
        send, own, kept, tables, solve_tables = pl.pallas_call(
            pack_kernel,
            in_specs=[hbm, hbm, hbm, vmem],
            out_shape=(
                message,
                jax.ShapeDtypeStruct(((KRYLOV + 1) * ROWS, LANES), jnp.float32),
                jax.ShapeDtypeStruct(resid.shape, jnp.float32),
                jax.ShapeDtypeStruct((2, 2, cols // 2, cols // 2), jnp.bfloat16),
                jax.ShapeDtypeStruct(solve_tables.shape, jnp.bfloat16),
            ),
            scratch_shapes=[
                pltpu.VMEM(basis.shape, jnp.float32),
                pltpu.SemaphoreType.DMA((3,)),
            ],
            compiler_params=params,
            name="pack",
        )(*placed, lent)
        recv = lax.all_to_all(send, axes, 0, 0, tiled=True)
        back = pl.pallas_call(
            lambda *refs: solve_kernel(kappa, count, steps, cols, *refs),
            out_shape=message,
            compiler_params=params,
            name="solve",
        )(recv, own, solve_tables)
        home = lax.all_to_all(back, axes, 0, 0, tiled=True)
        shard = jax.ShapeDtypeStruct(resid.shape, jnp.float32)
        precond, image, gram = pl.pallas_call(
            unpack_kernel,
            out_shape=(shard, shard, jax.ShapeDtypeStruct((KRYLOV + 1,), jnp.float32)),
            out_specs=(vmem, vmem, pl.BlockSpec(memory_space=pltpu.SMEM)),
            compiler_params=params,
            name="unpack",
        )(home, kept, tables)
        return precond, image, gram

    return jax.shard_map(
        on_device,
        mesh=mesh,
        in_specs=(P(None, "tm", "rows", None), P(None, None, "tm", "rows", None)),
        out_specs=(P(None, "tm", "rows", None), P(None, "tm", "rows", None), P()),
        check_vma=False,
    )
```
